32 devices in a mesh: slab: 16 (over z, x, core), tile: 2 (over y).
Axes of the slice: x: 2, y: 2, z: 4, core: 2. Of those that a mesh axis runs over, the one named last changes fastest.
Arguments:
- features: bfloat16 [16, 2, 512, 128], P('slab', 'tile'), may hold values from -24 to 24
- counts: int32 [16, 2], P('slab', 'tile'), may hold values from 128 to 512, as said below
- rulebook: int32 [16, 2, 27, 512], P('slab', 'tile'), may hold values from 0 to 800, as said below
- face_rows: int32 [16, 2, 4, 64], P('slab', 'tile'), may hold values from 0 to 511, as said below
- conv_one: bfloat16 [27, 128, 128], replicated, may hold values from -0.109375 to 0.109375
- gain_one: float32 [128], replicated, may hold values from 0.5 to 1.5
- shift_one: float32 [128], replicated, may hold values from -0.5 to 0.5
- conv_two: bfloat16 [27, 128, 128], replicated, may hold values from -0.109375 to 0.109375
- gain_two: float32 [128], replicated, may hold values from 0.5 to 1.5
- shift_two: float32 [128], replicated, may hold values from -0.5 to 0.5
Outputs:
- output: bfloat16 [16, 2, 512, 128], P('slab', 'tile')
The draws below stay inside these ranges and needn't reach their ends.
Inputs may be any that keep to these rules, and one draw needn't show every extreme that they name: `counts`: each device's voxels fill its 8 x 8 grid columns with the same number each, between 2 and 8; some device of the highest slab index holds 512. `rulebook`: an entry names the extended-table row that holds the voxel's neighbour at offset k = 9 (dx + 1) + 3 (dy + 1) + (dz + 1) of the submanifold 3x3x3 stencil, or 800 where that cell is inactive or outside the grid; the voxel itself is at offset 13; rows at or past the device's count name 800 at every offset. `face_rows`: lists 0 to 3 hold the device's voxels on its lower and higher face along the first, then the lower and higher face along the second dimension; the j-th voxel of the i-th column along a face stands at position i * 8 + j; unused positions name row 0.
All inputs are finite; a program needn't handle non-finite values.
Results may differ from the reference program's by a relative error of at most 0.0033.
Values may be sent and summed in bfloat16 or wider, within the bound.
A program may use at most 64 MiB of HBM per device.

```python
import math
import jax
import jax.numpy as jnp
from jax import lax

CHANNELS = 128
SIDE = 8
COLUMN = 8
DEPTH = 512
ROWS = 512
FACE = 64
TABLE = 800
N_SLAB = 16
N_TILE = 2


def voxel_layout(key):
    base_key = jax.random.fold_in(key, 11)
    coin_key, pick_key, depth_key = jax.random.split(base_key, 3)
    quarter = COLUMN // 4
    slab_ramp = quarter + (COLUMN - quarter) * jnp.arange(N_SLAB, dtype=jnp.int32) // max(N_SLAB - 1, 1)
    coin_flip = jax.random.randint(coin_key, (N_SLAB, N_TILE), 0, 2)
    per_column = jnp.where(coin_flip == 0, slab_ramp[:, None], quarter).astype(jnp.int32)
    chosen = jax.random.randint(pick_key, (), 0, N_TILE)
    per_column = per_column.at[N_SLAB - 1, chosen].set(COLUMN)
    column_total = N_SLAB * N_TILE * SIDE * SIDE
    depth_keys = jax.random.split(depth_key, column_total)
    shuffled = jax.vmap(lambda one_key: jax.random.permutation(one_key, DEPTH)[:COLUMN])(depth_keys)
    shuffled = shuffled.astype(jnp.int32).reshape(N_SLAB, N_TILE, SIDE, SIDE, COLUMN)
    rank_list = jnp.arange(COLUMN, dtype=jnp.int32)
    full_shape = (N_SLAB, N_TILE, SIDE, SIDE, COLUMN)
    own_count = jnp.broadcast_to(per_column[:, :, None, None, None], full_shape)
    filled = jnp.broadcast_to(rank_list, full_shape) < own_count
    depth_pos = jnp.sort(jnp.where(filled, shuffled, DEPTH + COLUMN), axis=-1)
    local_slab = jnp.broadcast_to(jnp.arange(SIDE, dtype=jnp.int32)[None, None, :, None, None], full_shape)
    local_tile = jnp.broadcast_to(jnp.arange(SIDE, dtype=jnp.int32)[None, None, None, :, None], full_shape)
    slab_index = jnp.broadcast_to(jnp.arange(N_SLAB, dtype=jnp.int32)[:, None, None, None, None], full_shape)
    tile_index = jnp.broadcast_to(jnp.arange(N_TILE, dtype=jnp.int32)[None, :, None, None, None], full_shape)
    slab_cell = slab_index * SIDE + local_slab
    tile_cell = tile_index * SIDE + local_tile
    rank_full = jnp.broadcast_to(rank_list, full_shape)
    occupancy = jnp.full((N_SLAB * SIDE, N_TILE * SIDE, DEPTH), -1, jnp.int32)
    occupancy = occupancy.at[slab_cell, tile_cell, depth_pos].set(rank_full, mode='drop')
    tap_values = []
    for shift_slab in range(-1, 2):
        for shift_tile in range(-1, 2):
            for shift_depth in range(-1, 2):
                near_slab = local_slab + shift_slab
                near_tile = local_tile + shift_tile
                near_depth = depth_pos + shift_depth
                cell_slab = slab_cell + shift_slab
                cell_tile = tile_cell + shift_tile
                inside = (cell_slab >= 0) & (cell_slab < N_SLAB * SIDE) & (cell_tile >= 0) & (cell_tile < N_TILE * SIDE)
                inside = inside & (near_depth >= 0) & (near_depth < DEPTH) & filled
                found_rank = occupancy[jnp.clip(cell_slab, 0, N_SLAB * SIDE - 1), jnp.clip(cell_tile, 0, N_TILE * SIDE - 1), jnp.clip(near_depth, 0, DEPTH - 1)]
                present = inside & (found_rank >= 0)
                in_slab = (near_slab >= 0) & (near_slab < SIDE)
                in_tile = (near_tile >= 0) & (near_tile < SIDE)
                own_index = (near_slab * SIDE + near_tile) * own_count + found_rank
                slab_index_low = ROWS + near_tile * COLUMN + found_rank
                slab_index_high = ROWS + FACE + near_tile * COLUMN + found_rank
                tile_index_low = ROWS + 2 * FACE + (near_slab + 1) * COLUMN + found_rank
                tile_index_high = ROWS + 3 * FACE + 2 * COLUMN + (near_slab + 1) * COLUMN + found_rank
                local_index = jnp.where(in_slab & in_tile, own_index, jnp.where(in_tile, jnp.where(near_slab < 0, slab_index_low, slab_index_high), jnp.where(near_tile < 0, tile_index_low, tile_index_high)))
                tap_values.append(jnp.where(present, local_index, TABLE).astype(jnp.int32))
    stacked = jnp.stack(tap_values, axis=2)
    big_shape = (N_SLAB, N_TILE, 27, SIDE, SIDE, COLUMN)
    row_target = jnp.where(filled, (local_slab * SIDE + local_tile) * own_count + rank_full, ROWS)
    row_target = jnp.broadcast_to(row_target[:, :, None], big_shape)
    slab_target = jnp.broadcast_to(slab_index[:, :, None], big_shape)
    tile_target = jnp.broadcast_to(tile_index[:, :, None], big_shape)
    tap_target = jnp.broadcast_to(jnp.arange(27, dtype=jnp.int32)[None, None, :, None, None, None], big_shape)
    rulebook = jnp.full((N_SLAB, N_TILE, 27, ROWS), TABLE, jnp.int32)
    rulebook = rulebook.at[slab_target, tile_target, tap_target, row_target].set(stacked, mode='drop')
    along_face = jnp.arange(SIDE, dtype=jnp.int32)[None, None, :, None]
    face_rank = rank_list[None, None, None, :]
    face_count = per_column[:, :, None, None]
    face_filled = face_rank < face_count
    slab_lower = (0 * SIDE + along_face) * face_count + face_rank
    slab_upper = ((SIDE - 1) * SIDE + along_face) * face_count + face_rank
    tile_lower = (along_face * SIDE + 0) * face_count + face_rank
    tile_upper = (along_face * SIDE + SIDE - 1) * face_count + face_rank
    face_lists = []
    for face_list in (slab_lower, slab_upper, tile_lower, tile_upper):
        face_lists.append(jnp.where(face_filled, face_list, 0).reshape(N_SLAB, N_TILE, FACE))
    face_rows = jnp.stack(face_lists, axis=2).astype(jnp.int32)
    counts = (per_column * SIDE * SIDE).astype(jnp.int32)
    return (counts, rulebook, face_rows)


def draw_counts(key, part):
    return voxel_layout(key)[0]


def draw_rulebook(key, part):
    return voxel_layout(key)[1]


def draw_face_rows(key, part):
    return voxel_layout(key)[2]


def draw_features(key, part):
    noise_key, row_key, chan_key = jax.random.split(jax.random.fold_in(key, 23), 3)
    array_shape = (N_SLAB, N_TILE, ROWS, CHANNELS)
    row_scale = jnp.exp(jax.random.uniform(row_key, (N_SLAB, N_TILE, ROWS, 1), jnp.float32, math.log(0.3), math.log(3.0)))
    chan_scale = jnp.exp(jax.random.uniform(chan_key, (CHANNELS,), jnp.float32, math.log(0.5), math.log(2.0)))
    base_noise = jnp.clip(jax.random.normal(noise_key, array_shape, jnp.float32), -4.0, 4.0)
    return (base_noise * row_scale * chan_scale).astype(jnp.bfloat16)


def gaussian(own_key, extent, spread, limit, held_as=jnp.bfloat16):
    return jnp.clip(spread * jax.random.normal(own_key, extent, jnp.float32), -limit, limit).astype(held_as)


def setup_inputs(seed: int = 0) -> dict:
    streams_of = jax.random.split(jax.random.key(seed), 11)
    return {
        "features": draw_features(jax.random.fold_in(streams_of[10], 71), 0),
        "counts": draw_counts(jax.random.fold_in(streams_of[10], 71), 0),
        "rulebook": draw_rulebook(jax.random.fold_in(streams_of[10], 71), 0),
        "face_rows": draw_face_rows(jax.random.fold_in(streams_of[10], 71), 0),
        "conv_one": gaussian(streams_of[4], (27, CHANNELS, CHANNELS), (27 * CHANNELS) ** -0.5, 0.109375),
        "gain_one": jnp.clip(1.0 + 0.1 * jax.random.normal(streams_of[5], (CHANNELS,), jnp.float32), 0.5, 1.5),
        "shift_one": jnp.clip(jax.random.uniform(streams_of[6], (CHANNELS,), jnp.float32, -0.5, 0.5), -0.5, 0.5),
        "conv_two": gaussian(streams_of[7], (27, CHANNELS, CHANNELS), (27 * CHANNELS) ** -0.5, 0.109375),
        "gain_two": jnp.clip(1.0 + 0.1 * jax.random.normal(streams_of[8], (CHANNELS,), jnp.float32), 0.5, 1.5),
        "shift_two": jnp.clip(jax.random.uniform(streams_of[9], (CHANNELS,), jnp.float32, -0.5, 0.5), -0.5, 0.5),
    }


EPSILON = 1e-05

def extend(voxel_rows, face_rows):
    picked = jax.vmap(jax.vmap(lambda row_list, positions: row_list[positions]))(voxel_rows, face_rows)
    blank = jnp.zeros_like(picked[:1, :, 0])
    slab_low = jnp.concatenate([blank, picked[:-1, :, 1]], axis=0)
    slab_high = jnp.concatenate([picked[1:, :, 0], blank], axis=0)
    lower_send = jnp.concatenate([slab_low[:, :, :COLUMN], picked[:, :, 2], slab_high[:, :, :COLUMN]], axis=2)
    upper_send = jnp.concatenate([slab_low[:, :, FACE - COLUMN:], picked[:, :, 3], slab_high[:, :, FACE - COLUMN:]], axis=2)
    edge_rows = jnp.zeros_like(lower_send[:, :1])
    tile_low = jnp.concatenate([edge_rows, upper_send[:, :-1]], axis=1)
    tile_high = jnp.concatenate([lower_send[:, 1:], edge_rows], axis=1)
    zero_row = jnp.zeros_like(voxel_rows[:, :, :1])
    return jnp.concatenate([voxel_rows, slab_low, slab_high, tile_low, tile_high, zero_row], axis=2)

def convolve_all(lookup, rulebook, weight):
    device_count = N_SLAB * N_TILE
    flat_weight = weight.astype(jnp.float32).reshape(27 * CHANNELS, CHANNELS)
    tables = lookup.reshape(device_count, TABLE + 1, CHANNELS)
    indices = rulebook.reshape(device_count, 27, ROWS)

    def one_device(pair):
        table_rows, tap_rows = pair
        gathered = table_rows[tap_rows.T].reshape(ROWS, 27 * CHANNELS).astype(jnp.float32)
        return jnp.dot(gathered, flat_weight, preferred_element_type=jnp.float32)
    result = lax.map(one_device, (tables, indices))
    return result.reshape(N_SLAB, N_TILE, ROWS, CHANNELS)

def normalize(conv_out, live_mask, voxel_total, gain, shift):
    average = lax.optimization_barrier(jnp.sum(conv_out * live_mask, axis=(0, 1, 2))) / voxel_total
    centred = (conv_out - average) * live_mask
    variance = lax.optimization_barrier(jnp.sum(centred * centred, axis=(0, 1, 2))) / voxel_total
    return (conv_out - average) / jnp.sqrt(variance + EPSILON) * gain + shift

def reference(features, counts, rulebook, face_rows, conv_one, gain_one, shift_one, conv_two, gain_two, shift_two):
    live_mask = (jnp.arange(ROWS, dtype=jnp.int32)[None, None, :] < counts[:, :, None]).astype(jnp.float32)[..., None]
    voxel_total = jnp.sum(counts).astype(jnp.float32)
    first = convolve_all(extend(features, face_rows), rulebook, conv_one)
    hidden = (live_mask * jnp.maximum(normalize(first, live_mask, voxel_total, gain_one, shift_one), 0.0)).astype(jnp.bfloat16)
    second = convolve_all(extend(hidden, face_rows), rulebook, conv_two)
    summed = normalize(second, live_mask, voxel_total, gain_two, shift_two) + features.astype(jnp.float32)
    return (live_mask * jnp.maximum(summed, 0.0)).astype(jnp.bfloat16)
```

```python
from functools import partial

import jax
import jax.numpy as jnp
from jax import lax
from jax.experimental import pallas as pl
from jax.experimental.pallas import tpu as pltpu
from jax.sharding import PartitionSpec as P

SIDE = 8
EPSILON = 1e-05
MESH = pl.DeviceIdType.MESH
BLOCK = 256
PIECE = 16
F32 = jnp.float32
BF16 = jnp.bfloat16


def transfers(face_len):
    low, high = 0, face_len
    edge = face_len - PIECE
    end = PIECE + face_len
    return (
        (1, 0, high, face_len, 0, 0),
        (-1, 0, low, face_len, 0, face_len),
        (0, 1, 3 * face_len, face_len, 1, PIECE),
        (0, -1, 2 * face_len, face_len, 2, PIECE),
        (1, 1, high + edge, PIECE, 1, 0),
        (-1, 1, low + edge, PIECE, 1, end),
        (1, -1, high, PIECE, 2, 0),
        (-1, -1, low, PIECE, 2, end),
    )


def block_kernel(
    n_slab,
    n_tile,
    feat_hbm,
    count_ref,
    rule_hbm,
    face_hbm,
    gain_one_hbm,
    shift_one_hbm,
    gain_two_hbm,
    shift_two_hbm,
    conv_one_ref,
    conv_two_ref,
    out_ref,
    feat_ref,
    rule_ref,
    face_ref,
    gain_one_ref,
    shift_one_ref,
    gain_two_ref,
    shift_two_ref,
    weight_ref,
    weight_t_ref,
    onehot_ref,
    part_ref,
    keep_ref,
    face_hot_ref,
    square_ref,
    slope_ref,
    own_ref,
    send_ref,
    wide_send_ref,
    halo_ref,
    wide_halo_ref,
    lhs_ref,
    picked_ref,
    stats_ref,
    counts_ref,
    input_sem,
    send_sem,
    recv_sem,
    stat_send_sem,
    stat_recv_sem,
):
    rows, channels = feat_ref.shape
    taps = rule_ref.shape[0]
    face_len = face_ref.shape[1]
    column = face_len // SIDE
    n_dev = n_slab * n_tile
    blocks = rows // BLOCK
    group = taps // 3
    slab = lax.axis_index("slab")
    tile = lax.axis_index("tile")
    me = slab * n_tile + tile

    def fetch(i, src, dst):
        return pltpu.make_async_copy(src, dst, input_sem.at[i])

    input_copies = [
        fetch(0, feat_hbm, feat_ref),
        fetch(1, face_hbm, face_ref),
        fetch(2, rule_hbm, rule_ref),
    ]
    affine_copies = [
        fetch(3, gain_one_hbm, gain_one_ref),
        fetch(4, shift_one_hbm, shift_one_ref),
        fetch(5, gain_two_hbm, gain_two_ref),
        fetch(6, shift_two_hbm, shift_two_ref),
    ]
    weight_copies = [
        fetch(7, conv_one_ref, weight_ref.at[0]),
        fetch(8, conv_two_ref, weight_ref.at[1]),
    ]
    for copy in (input_copies[1], input_copies[0], input_copies[2]):
        copy.start()
    halo_ref[...] = jnp.zeros_like(halo_ref)
    wide_halo_ref[...] = jnp.zeros_like(wide_halo_ref)

    def moved(place, step, size):
        if size & (size - 1) == 0:
            return place ^ step
        place = place + step
        return jnp.where(place >= size, place - size, place)

    def each_peer(act):
        for j in reversed(range(n_tile)):
            other = moved(tile, j, n_tile) if j else tile

            def visit(i, carry):
                act({"slab": moved(slab, n_slab - 1 - i, n_slab), "tile": other})
                return carry

            last = n_slab if j else n_slab - 1
            lax.fori_loop(0, last, visit, 0, unroll=n_slab <= 16)

    barrier = pltpu.get_barrier_semaphore()

    each_peer(
        lambda peer: pl.semaphore_signal(
            barrier, inc=1, device_id=peer, device_id_type=MESH
        )
    )
    for copy in weight_copies + affine_copies:
        copy.start()

    def halo(which, start):
        source, target = ((send_ref, halo_ref), (wide_send_ref, wide_halo_ref))[which]
        for j, (ds, dt, first, size, buffer, place) in enumerate(transfers(face_len)):
            copy = pltpu.make_async_remote_copy(
                src_ref=source.at[pl.ds(first, size)],
                dst_ref=target.at[buffer, pl.ds(place, size)],
                send_sem=send_sem.at[which, j],
                recv_sem=recv_sem.at[which, j],
                device_id={"slab": slab + ds, "tile": tile + dt},
                device_id_type=MESH,
            )
            sends, receives = True, True
            if ds > 0:
                sends, receives = slab < n_slab - 1, slab > 0
            elif ds < 0:
                sends, receives = slab > 0, slab < n_slab - 1
            if dt > 0:
                sends, receives = sends & (tile < n_tile - 1), receives & (tile > 0)
            elif dt < 0:
                sends, receives = sends & (tile > 0), receives & (tile < n_tile - 1)
            if start:
                pl.when(sends)(copy.start)
            else:
                pl.when(receives)(copy.wait_recv)
                pl.when(sends)(copy.wait_send)

    input_copies[1].wait()
    square_ref[...] = jnp.zeros_like(square_ref)
    square_ref[0:4, 0:face_len] = face_ref[...].astype(F32)
    face_cols = square_ref[...].T
    lane_rows = lax.broadcasted_iota(jnp.int32, (face_len, rows), 1)
    for k in range(4):
        wanted = face_cols[0:face_len, k : k + 1].astype(jnp.int32)
        face_hot_ref[k * face_len : (k + 1) * face_len, :] = jnp.where(
            lane_rows == wanted, 1.0, 0.0
        ).astype(BF16)

    input_copies[0].wait()
    feat = feat_ref[...]
    send_ref[...] = jnp.dot(face_hot_ref[...], feat, preferred_element_type=F32).astype(BF16)

    input_copies[2].wait()
    rule = rule_ref[...]
    tile_len = face_len + 2 * column
    below = rows + 2 * face_len
    above = below + tile_len
    q_low = rule - below
    q_high = rule - above
    base = 2 * face_len + PIECE - column
    skip = PIECE - column
    place_low = base + q_low + jnp.where(q_low >= column + face_len, skip, 0)
    place_high = base + q_high - jnp.where(q_high < column, skip, 0)
    place = jnp.where(
        rule < rows,
        rule & (BLOCK - 1),
        jnp.where(
            rule < below, rule - rows, jnp.where(rule < above, place_low, place_high)
        ),
    )
    part = jnp.where(
        rule < rows, rule // BLOCK, jnp.where(rule < above + tile_len, blocks, blocks + 1)
    )
    part_ref[...] = part
    dead = (part > blocks) | ((rule < rows) & (rule >= count_ref[0, 0]))
    keep_ref[...] = jnp.where(dead, 0, 1)
    position = lax.broadcasted_iota(jnp.int32, (BLOCK, rows), 0).astype(F32).astype(BF16)
    place = place.astype(F32).astype(BF16)
    one, none = jnp.ones((BLOCK, rows), BF16), jnp.zeros((BLOCK, rows), BF16)
    for k in range(taps):
        onehot_ref[k] = jnp.where(position == place[k], one, none)

    count = count_ref[0, 0]
    live = (lax.broadcasted_iota(jnp.int32, (rows, 1), 0) < count).astype(F32)

    def share(which, buffer):
        mine = buffer.at[me]
        each_peer(
            lambda peer: pltpu.make_async_remote_copy(
                src_ref=mine,
                dst_ref=mine,
                send_sem=stat_send_sem.at[which],
                recv_sem=stat_recv_sem.at[which],
                device_id=peer,
                device_id_type=MESH,
            ).start()
        )

    def shared(which, buffer):
        others = buffer.at[pl.ds(0, n_dev - 1)]
        pltpu.make_async_copy(others, others, stat_recv_sem.at[which]).wait()
        pltpu.make_async_copy(others, others, stat_send_sem.at[which]).wait()
        return jnp.sum(buffer[...], axis=0)

    counts_ref[me] = jnp.full((1, channels), count.astype(F32))
    pl.semaphore_wait(barrier, n_dev - 1)
    halo(0, True)
    share(2, counts_ref)

    def load_local(values):
        for b in range(blocks):
            turned = values[b * BLOCK : (b + 1) * BLOCK].T
            for y in range(3):
                lhs_ref[y, b * channels : (b + 1) * channels, :] = turned

    def load_halo(pieces):
        turned = [piece.T for piece in pieces]
        low = blocks * channels
        half = BLOCK // 2
        for y, other in ((0, turned[1]), (1, None), (2, turned[2])):
            lhs_ref[y, low:, 0:half] = turned[0]
            lhs_ref[y, low:, half:] = jnp.zeros_like(turned[0]) if other is None else other

    load_local(feat)
    def turn_weights(i):
        weight_copies[i].wait()
        for x in range(3):
            weight_t_ref[i, x] = weight_ref[i, x * group * channels : (x + 1) * group * channels, :].T

    turn_weights(0)

    def choose(home, found, value, chosen):
        for i, b in enumerate(chosen):
            value = jnp.where(home == b, found[i * channels : (i + 1) * channels], value)
        return value

    def pick_local(x, carry):
        for j in range(group):
            tap = x * group + j
            found = jnp.dot(
                lhs_ref[0, 0 : blocks * channels], onehot_ref[tap], preferred_element_type=F32
            )
            value = choose(part_ref[tap], found, jnp.zeros((channels, rows), F32), range(blocks))
            picked_ref[tap] = value.astype(BF16)
        return carry

    def pick_halo(tap, j):
        found = jnp.dot(
            lhs_ref[j // 3, blocks * channels :], onehot_ref[tap], preferred_element_type=F32
        )
        value = choose(part_ref[tap], found, picked_ref[tap].astype(F32), (blocks,))
        picked_ref[tap] = value.astype(BF16)

    def pick_halos(x):
        for j in range(group):
            if x != 1 or j // 3 != 1:
                pick_halo(x * group + j, j)

    def multiply(which, x, total):
        taken = picked_ref[pl.ds(x * group, group)].reshape(group * channels, rows)
        return total + jnp.dot(weight_t_ref[which, x], taken, preferred_element_type=F32)

    def tell_sums(which, values):
        kept = values * live
        stats_ref[which, me] = jnp.concatenate(
            [
                jnp.sum(kept, axis=0, keepdims=True),
                jnp.sum(kept * values, axis=0, keepdims=True),
            ],
            axis=0,
        )
        share(which, stats_ref.at[which])
        return stats_ref[which, me][0:1] / count.astype(F32)

    def affine(which, voxels, gain_ref, shift_ref):
        total = shared(which, stats_ref.at[which])
        average = total[0:1] / voxels
        variance = total[1:2] / voxels - average * average
        scale = lax.rsqrt(variance + EPSILON) * gain_ref[...]
        return scale, shift_ref[...] - average * scale

    lax.fori_loop(0, 3, pick_local, 0)
    halo(0, False)
    load_halo([halo_ref[i] for i in range(3)])
    blank = jnp.zeros((channels, rows), F32)
    first = blank
    for x in range(3):
        pick_halos(x)
        first = multiply(0, x, first)
    first = first.T
    centre = tell_sums(0, first)
    coarse = first.astype(BF16)
    fine = (first - coarse.astype(F32)).astype(BF16)
    both = jnp.dot(
        face_hot_ref[...],
        jnp.concatenate([coarse, fine], axis=1),
        preferred_element_type=F32,
    )
    wide_send_ref[...] = both[:, 0:channels] + both[:, channels:]
    halo(1, True)
    centred = first - centre
    for b in range(blocks):
        turned = centred[b * BLOCK : (b + 1) * BLOCK].T
        own_ref[:, b * BLOCK : (b + 1) * BLOCK] = turned
        lhs_ref[0, b * channels : (b + 1) * channels, :] = turned.astype(BF16)
    lax.fori_loop(0, 3, pick_local, 0)
    turn_weights(1)
    halo(1, False)
    load_halo([(wide_halo_ref[i] - centre).astype(BF16) for i in range(3)])
    for x in range(3):
        pick_halos(x)
    for copy in affine_copies:
        copy.wait()
    voxels = shared(2, counts_ref)
    scale, offset = affine(0, voxels, gain_one_ref, shift_one_ref)

    square_ref[...] = jnp.broadcast_to(scale, (channels, channels)).T
    slope_ref[...] = jnp.broadcast_to(centre * scale + offset, (channels, channels)).T

    def convolve_two(x, total):
        slope = jnp.concatenate([square_ref[...]] * (rows // channels), axis=1)
        level = jnp.concatenate([slope_ref[...]] * (rows // channels), axis=1)
        for j in range(group):
            tap = x * group + j
            value = picked_ref[tap].astype(F32)
            if j == group // 2:
                middle = jnp.full((channels, rows), x, jnp.int32) == 1
                value = jnp.where(middle, own_ref[...], value)
            value = jnp.maximum(value * slope + level, 0.0)
            value = jnp.where(keep_ref[tap] > 0, value, 0.0)
            picked_ref[tap] = value.astype(BF16)
        return multiply(1, x, total)

    second = lax.fori_loop(0, 3, convolve_two, blank).T
    tell_sums(1, second)
    scale, offset = affine(1, voxels, gain_two_ref, shift_two_ref)
    summed = second * scale + offset + feat_ref[...].astype(F32)
    out_ref[...] = (live * jnp.maximum(summed, 0.0)).astype(BF16)


def per_device(
    n_slab,
    n_tile,
    features,
    counts,
    rulebook,
    face_rows,
    conv_one,
    gain_one,
    shift_one,
    conv_two,
    gain_two,
    shift_two,
):
    rows, channels = features.shape[2:]
    taps = rulebook.shape[2]
    faces, face_len = face_rows.shape[2:]
    blocks = rows // BLOCK
    smem = pl.BlockSpec(memory_space=pltpu.SMEM)
    vmem = pl.BlockSpec(memory_space=pltpu.VMEM)
    hbm = pl.BlockSpec(memory_space=pltpu.HBM)
    group = taps // 3 * channels
    output = pl.pallas_call(
        partial(block_kernel, n_slab, n_tile),
        out_shape=jax.ShapeDtypeStruct((rows, channels), features.dtype),
        in_specs=[hbm, smem] + [hbm] * 8,
        out_specs=vmem,
        scratch_shapes=[
            pltpu.VMEM((rows, channels), BF16),
            pltpu.VMEM((taps, 1, rows), jnp.int32),
            pltpu.VMEM((faces, face_len), jnp.int32),
            pltpu.VMEM((1, channels), F32),
            pltpu.VMEM((1, channels), F32),
            pltpu.VMEM((1, channels), F32),
            pltpu.VMEM((1, channels), F32),
            pltpu.VMEM((2, taps * channels, channels), BF16),
            pltpu.VMEM((2, 3, channels, group), BF16),
            pltpu.VMEM((taps, BLOCK, rows), BF16),
            pltpu.VMEM((taps, 1, rows), jnp.int32),
            pltpu.VMEM((taps, 1, rows), jnp.int32),
            pltpu.VMEM((faces * face_len, rows), BF16),
            pltpu.VMEM((channels, channels), F32),
            pltpu.VMEM((channels, channels), F32),
            pltpu.VMEM((channels, rows), F32),
            pltpu.VMEM((faces * face_len, channels), BF16),
            pltpu.VMEM((faces * face_len, channels), F32),
            pltpu.VMEM((3, BLOCK // 2, channels), BF16),
            pltpu.VMEM((3, BLOCK // 2, channels), F32),
            pltpu.VMEM((3, (blocks + 1) * channels, BLOCK), BF16),
            pltpu.VMEM((taps, channels, rows), BF16),
            pltpu.VMEM((2, n_slab * n_tile, 2, channels), F32),
            pltpu.VMEM((n_slab * n_tile, 1, channels), F32),
            pltpu.SemaphoreType.DMA((9,)),
            pltpu.SemaphoreType.DMA((2, 8)),
            pltpu.SemaphoreType.DMA((2, 8)),
            pltpu.SemaphoreType.DMA((3,)),
            pltpu.SemaphoreType.DMA((3,)),
        ],
        compiler_params=pltpu.CompilerParams(
            collective_id=0, has_side_effects=True, vmem_limit_bytes=30000000
        ),
    )(
        features[0, 0],
        counts,
        rulebook.reshape(taps, 1, rows),
        face_rows[0, 0],
        gain_one[None],
        shift_one[None],
        gain_two[None],
        shift_two[None],
        conv_one.reshape(taps * channels, channels),
        conv_two.reshape(taps * channels, channels),
    )
    return output[None, None]


def solution(mesh):
    placed = (
        P("slab", "tile", None, None),
        P("slab", "tile"),
        P("slab", "tile", None, None),
        P("slab", "tile", None, None),
        P(),
        P(),
        P(),
        P(),
        P(),
        P(),
    )
    return jax.shard_map(
        partial(per_device, mesh.shape["slab"], mesh.shape["tile"]),
        mesh=mesh,
        in_specs=placed,
        out_specs=P("slab", "tile", None, None),
        check_vma=False,
    )
```

```python
from functools import partial

import jax
import jax.numpy as jnp
from jax import lax
from jax.experimental import pallas as pl
from jax.experimental.pallas import tpu as pltpu
from jax.sharding import PartitionSpec as P

SIDE = 8
EPSILON = 1e-05
MESH = pl.DeviceIdType.MESH
BLOCK = 256
PIECE = 16
F32 = jnp.float32
BF16 = jnp.bfloat16


def transfers(face_len):
    low, high = 0, face_len
    edge = face_len - PIECE
    end = PIECE + face_len
    return (
        (1, 0, high, face_len, 0, 0),
        (-1, 0, low, face_len, 0, face_len),
        (0, 1, 3 * face_len, face_len, 1, PIECE),
        (0, -1, 2 * face_len, face_len, 2, PIECE),
        (1, 1, high + edge, PIECE, 1, 0),
        (-1, 1, low + edge, PIECE, 1, end),
        (1, -1, high, PIECE, 2, 0),
        (-1, -1, low, PIECE, 2, end),
    )


def block_kernel(
    n_slab,
    n_tile,
    feat_hbm,
    count_ref,
    rule_hbm,
    face_hbm,
    gain_one_hbm,
    shift_one_hbm,
    gain_two_hbm,
    shift_two_hbm,
    conv_one_ref,
    conv_two_ref,
    out_ref,
    feat_ref,
    rule_ref,
    face_ref,
    gain_one_ref,
    shift_one_ref,
    gain_two_ref,
    shift_two_ref,
    weight_ref,
    weight_t_ref,
    onehot_ref,
    part_ref,
    keep_ref,
    face_hot_ref,
    square_ref,
    slope_ref,
    own_ref,
    send_ref,
    wide_send_ref,
    halo_ref,
    wide_halo_ref,
    lhs_ref,
    picked_ref,
    stats_ref,
    counts_ref,
    input_sem,
    send_sem,
    recv_sem,
    stat_send_sem,
    stat_recv_sem,
):
    rows, channels = feat_ref.shape
    taps = rule_ref.shape[0]
    face_len = face_ref.shape[1]
    column = face_len // SIDE
    n_dev = n_slab * n_tile
    blocks = rows // BLOCK
    group = taps // 3
    slab = lax.axis_index("slab")
    tile = lax.axis_index("tile")
    me = slab * n_tile + tile

    def fetch(i, src, dst):
        return pltpu.make_async_copy(src, dst, input_sem.at[i])

    input_copies = [
        fetch(0, feat_hbm, feat_ref),
        fetch(1, face_hbm, face_ref),
        fetch(2, rule_hbm, rule_ref),
    ]
    affine_copies = [
        fetch(3, gain_one_hbm, gain_one_ref),
        fetch(4, shift_one_hbm, shift_one_ref),
        fetch(5, gain_two_hbm, gain_two_ref),
        fetch(6, shift_two_hbm, shift_two_ref),
    ]
    weight_copies = [
        fetch(7, conv_one_ref, weight_ref.at[0]),
        fetch(8, conv_two_ref, weight_ref.at[1]),
    ]
    for copy in (input_copies[1], input_copies[0], input_copies[2]):
        copy.start()
    halo_ref[...] = jnp.zeros_like(halo_ref)
    wide_halo_ref[...] = jnp.zeros_like(wide_halo_ref)

    def moved(place, step, size):
        if size & (size - 1) == 0:
            return place ^ step
        place = place + step
        return jnp.where(place >= size, place - size, place)

    def each_peer(act):
        for j in reversed(range(n_tile)):
            other = moved(tile, j, n_tile) if j else tile

            def visit(i, carry):
                act({"slab": moved(slab, n_slab - 1 - i, n_slab), "tile": other})
                return carry

            last = n_slab if j else n_slab - 1
            lax.fori_loop(0, last, visit, 0, unroll=n_slab <= 16)

    barrier = pltpu.get_barrier_semaphore()

    each_peer(
        lambda peer: pl.semaphore_signal(
            barrier, inc=1, device_id=peer, device_id_type=MESH
        )
    )
    for copy in weight_copies + affine_copies:
        copy.start()

    def halo(which, start):
        source, target = ((send_ref, halo_ref), (wide_send_ref, wide_halo_ref))[which]
        for j, (ds, dt, first, size, buffer, place) in enumerate(transfers(face_len)):
            copy = pltpu.make_async_remote_copy(
                src_ref=source.at[pl.ds(first, size)],
                dst_ref=target.at[buffer, pl.ds(place, size)],
                send_sem=send_sem.at[which, j],
                recv_sem=recv_sem.at[which, j],
                device_id={"slab": slab + ds, "tile": tile + dt},
                device_id_type=MESH,
            )
            sends, receives = True, True
            if ds > 0:
                sends, receives = slab < n_slab - 1, slab > 0
            elif ds < 0:
                sends, receives = slab > 0, slab < n_slab - 1
            if dt > 0:
                sends, receives = sends & (tile < n_tile - 1), receives & (tile > 0)
            elif dt < 0:
                sends, receives = sends & (tile > 0), receives & (tile < n_tile - 1)
            if start:
                pl.when(sends)(copy.start)
            else:
                pl.when(receives)(copy.wait_recv)
                pl.when(sends)(copy.wait_send)

    input_copies[1].wait()
    square_ref[...] = jnp.zeros_like(square_ref)
    square_ref[0:4, 0:face_len] = face_ref[...].astype(F32)
    face_cols = square_ref[...].T
    lane_rows = lax.broadcasted_iota(jnp.int32, (face_len, rows), 1)
    for k in range(4):
        wanted = face_cols[0:face_len, k : k + 1].astype(jnp.int32)
        face_hot_ref[k * face_len : (k + 1) * face_len, :] = jnp.where(
            lane_rows == wanted, 1.0, 0.0
        ).astype(BF16)

    input_copies[0].wait()
    feat = feat_ref[...]
    send_ref[...] = jnp.dot(face_hot_ref[...], feat, preferred_element_type=F32).astype(BF16)

    input_copies[2].wait()
    rule = rule_ref[...]
    tile_len = face_len + 2 * column
    below = rows + 2 * face_len
    above = below + tile_len
    q_low = rule - below
    q_high = rule - above
    base = 2 * face_len + PIECE - column
    skip = PIECE - column
    place_low = base + q_low + jnp.where(q_low >= column + face_len, skip, 0)
    place_high = base + q_high - jnp.where(q_high < column, skip, 0)
    place = jnp.where(
        rule < rows,
        rule & (BLOCK - 1),
        jnp.where(
            rule < below, rule - rows, jnp.where(rule < above, place_low, place_high)
        ),
    )
    part = jnp.where(
        rule < rows, rule // BLOCK, jnp.where(rule < above + tile_len, blocks, blocks + 1)
    )
    part_ref[...] = part
    dead = (part > blocks) | ((rule < rows) & (rule >= count_ref[0, 0]))
    keep_ref[...] = jnp.where(dead, 0, 1)
    position = lax.broadcasted_iota(jnp.int32, (BLOCK, rows), 0).astype(F32).astype(BF16)
    place = place.astype(F32).astype(BF16)
    one, none = jnp.ones((BLOCK, rows), BF16), jnp.zeros((BLOCK, rows), BF16)
    for k in range(taps):
        onehot_ref[k] = jnp.where(position == place[k], one, none)

    count = count_ref[0, 0]
    live = (lax.broadcasted_iota(jnp.int32, (rows, 1), 0) < count).astype(F32)

    def share(which, buffer):
        mine = buffer.at[me]
        each_peer(
            lambda peer: pltpu.make_async_remote_copy(
                src_ref=mine,
                dst_ref=mine,
                send_sem=stat_send_sem.at[which],
                recv_sem=stat_recv_sem.at[which],
                device_id=peer,
                device_id_type=MESH,
            ).start()
        )

    def shared(which, buffer):
        others = buffer.at[pl.ds(0, n_dev - 1)]
        pltpu.make_async_copy(others, others, stat_recv_sem.at[which]).wait()
        pltpu.make_async_copy(others, others, stat_send_sem.at[which]).wait()
        return jnp.sum(buffer[...], axis=0)

    counts_ref[me] = jnp.full((1, channels), count.astype(F32))
    pl.semaphore_wait(barrier, n_dev - 1)
    halo(0, True)
    share(2, counts_ref)

    def load_local(values):
        for b in range(blocks):
            turned = values[b * BLOCK : (b + 1) * BLOCK].T
            for y in range(3):
                lhs_ref[y, b * channels : (b + 1) * channels, :] = turned

    def load_halo(pieces):
        turned = [piece.T for piece in pieces]
        low = blocks * channels
        half = BLOCK // 2
        for y, other in ((0, turned[1]), (1, None), (2, turned[2])):
            lhs_ref[y, low:, 0:half] = turned[0]
            lhs_ref[y, low:, half:] = jnp.zeros_like(turned[0]) if other is None else other

    load_local(feat)
    def turn_weights(i):
        weight_copies[i].wait()
        for x in range(3):
            weight_t_ref[i, x] = weight_ref[i, x * group * channels : (x + 1) * group * channels, :].T

    turn_weights(0)

    def choose(home, found, value, chosen):
        for i, b in enumerate(chosen):
            value = jnp.where(home == b, found[i * channels : (i + 1) * channels], value)
        return value

    def pick_local(x, carry):
        for j in range(group):
            tap = x * group + j
            found = jnp.dot(
                lhs_ref[0, 0 : blocks * channels], onehot_ref[tap], preferred_element_type=F32
            )
            value = choose(part_ref[tap], found, jnp.zeros((channels, rows), F32), range(blocks))
            picked_ref[tap] = value.astype(BF16)
        return carry

    def pick_halo(tap, j):
        found = jnp.dot(
            lhs_ref[j // 3, blocks * channels :], onehot_ref[tap], preferred_element_type=F32
        )
        value = choose(part_ref[tap], found, picked_ref[tap].astype(F32), (blocks,))
        picked_ref[tap] = value.astype(BF16)

    def pick_halos(x):
        for j in range(group):
            if x != 1 or j // 3 != 1:
                pick_halo(x * group + j, j)

    def multiply(which, x, total):
        taken = picked_ref[pl.ds(x * group, group)].reshape(group * channels, rows)
        return total + jnp.dot(weight_t_ref[which, x], taken, preferred_element_type=F32)

    def tell_sums(which, values):
        kept = values * live
        stats_ref[which, me] = jnp.concatenate(
            [
                jnp.sum(kept, axis=0, keepdims=True),
                jnp.sum(kept * values, axis=0, keepdims=True),
            ],
            axis=0,
        )
        share(which, stats_ref.at[which])
        return stats_ref[which, me][0:1] / count.astype(F32)

    def affine(which, voxels, gain_ref, shift_ref):
        total = shared(which, stats_ref.at[which])
        average = total[0:1] / voxels
        variance = total[1:2] / voxels - average * average
        scale = lax.rsqrt(variance + EPSILON) * gain_ref[...]
        return scale, shift_ref[...] - average * scale

    lax.fori_loop(0, 3, pick_local, 0)
    halo(0, False)
    load_halo([halo_ref[i] for i in range(3)])
    blank = jnp.zeros((channels, rows), F32)
    first = blank
    for x in range(3):
        pick_halos(x)
        first = multiply(0, x, first)
    first = first.T
    centre = tell_sums(0, first)
    coarse = first.astype(BF16)
    fine = (first - coarse.astype(F32)).astype(BF16)
    both = jnp.dot(
        face_hot_ref[...],
        jnp.concatenate([coarse, fine], axis=1),
        preferred_element_type=F32,
    )
    wide_send_ref[...] = both[:, 0:channels] + both[:, channels:]
    halo(1, True)
    centred = first - centre
    for b in range(blocks):
        turned = centred[b * BLOCK : (b + 1) * BLOCK].T
        own_ref[:, b * BLOCK : (b + 1) * BLOCK] = turned
        lhs_ref[0, b * channels : (b + 1) * channels, :] = turned.astype(BF16)
    lax.fori_loop(0, 3, pick_local, 0)
    turn_weights(1)
    halo(1, False)
    load_halo([(wide_halo_ref[i] - centre).astype(BF16) for i in range(3)])
    for x in range(3):
        pick_halos(x)
    for copy in affine_copies:
        copy.wait()
    voxels = shared(2, counts_ref)
    scale, offset = affine(0, voxels, gain_one_ref, shift_one_ref)

    square_ref[...] = jnp.broadcast_to(scale, (channels, channels)).T
    slope_ref[...] = jnp.broadcast_to(centre * scale + offset, (channels, channels)).T

    def convolve_two(x, total):
        slope = jnp.concatenate([square_ref[...]] * (rows // channels), axis=1)
        level = jnp.concatenate([slope_ref[...]] * (rows // channels), axis=1)
        for j in range(group):
            tap = x * group + j
            value = picked_ref[tap].astype(F32)
            if j == group // 2:
                middle = jnp.full((channels, rows), x, jnp.int32) == 1
                value = jnp.where(middle, own_ref[...], value)
            value = jnp.maximum(value * slope + level, 0.0)
            value = jnp.where(keep_ref[tap] > 0, value, 0.0)
            picked_ref[tap] = value.astype(BF16)
        return multiply(1, x, total)

    second = lax.fori_loop(0, 3, convolve_two, blank).T
    tell_sums(1, second)
    scale, offset = affine(1, voxels, gain_two_ref, shift_two_ref)
    summed = second * scale + offset + feat_ref[...].astype(F32)
    out_ref[...] = (live * jnp.maximum(summed, 0.0)).astype(BF16)


def per_device(
    n_slab,
    n_tile,
    features,
    counts,
    rulebook,
    face_rows,
    conv_one,
    gain_one,
    shift_one,
    conv_two,
    gain_two,
    shift_two,
):
    rows, channels = features.shape[2:]
    taps = rulebook.shape[2]
    faces, face_len = face_rows.shape[2:]
    blocks = rows // BLOCK
    smem = pl.BlockSpec(memory_space=pltpu.SMEM)
    vmem = pl.BlockSpec(memory_space=pltpu.VMEM)
    hbm = pl.BlockSpec(memory_space=pltpu.HBM)
    group = taps // 3 * channels
    stay = partial(pltpu.with_memory_space_constraint, memory_space=pltpu.HBM)
    output = pl.pallas_call(
        partial(block_kernel, n_slab, n_tile),
        out_shape=pltpu.VMEM((rows, channels), features.dtype),
        in_specs=[hbm, smem] + [hbm] * 8,
        out_specs=vmem,
        scratch_shapes=[
            pltpu.VMEM((rows, channels), BF16),
            pltpu.VMEM((taps, 1, rows), jnp.int32),
            pltpu.VMEM((faces, face_len), jnp.int32),
            pltpu.VMEM((1, channels), F32),
            pltpu.VMEM((1, channels), F32),
            pltpu.VMEM((1, channels), F32),
            pltpu.VMEM((1, channels), F32),
            pltpu.VMEM((2, taps * channels, channels), BF16),
            pltpu.VMEM((2, 3, channels, group), BF16),
            pltpu.VMEM((taps, BLOCK, rows), BF16),
            pltpu.VMEM((taps, 1, rows), jnp.int32),
            pltpu.VMEM((taps, 1, rows), jnp.int32),
            pltpu.VMEM((faces * face_len, rows), BF16),
            pltpu.VMEM((channels, channels), F32),
            pltpu.VMEM((channels, channels), F32),
            pltpu.VMEM((channels, rows), F32),
            pltpu.VMEM((faces * face_len, channels), BF16),
            pltpu.VMEM((faces * face_len, channels), F32),
            pltpu.VMEM((3, BLOCK // 2, channels), BF16),
            pltpu.VMEM((3, BLOCK // 2, channels), F32),
            pltpu.VMEM((3, (blocks + 1) * channels, BLOCK), BF16),
            pltpu.VMEM((taps, channels, rows), BF16),
            pltpu.VMEM((2, n_slab * n_tile, 2, channels), F32),
            pltpu.VMEM((n_slab * n_tile, 1, channels), F32),
            pltpu.SemaphoreType.DMA((9,)),
            pltpu.SemaphoreType.DMA((2, 8)),
            pltpu.SemaphoreType.DMA((2, 8)),
            pltpu.SemaphoreType.DMA((3,)),
            pltpu.SemaphoreType.DMA((3,)),
        ],
        compiler_params=pltpu.CompilerParams(
            collective_id=0, has_side_effects=True, vmem_limit_bytes=40000000
        ),
    )(
        stay(features[0, 0]),
        counts,
        stay(rulebook.reshape(taps, 1, rows)),
        stay(face_rows[0, 0]),
        stay(gain_one[None]),
        stay(shift_one[None]),
        stay(gain_two[None]),
        stay(shift_two[None]),
        stay(conv_one.reshape(taps * channels, channels)),
        stay(conv_two.reshape(taps * channels, channels)),
    )
    return output[None, None]


def solution(mesh):
    placed = (
        P("slab", "tile", None, None),
        P("slab", "tile"),
        P("slab", "tile", None, None),
        P("slab", "tile", None, None),
        P(),
        P(),
        P(),
        P(),
        P(),
        P(),
    )
    return jax.shard_map(
        partial(per_device, mesh.shape["slab"], mesh.shape["tile"]),
        mesh=mesh,
        in_specs=placed,
        out_specs=P("slab", "tile", None, None),
        check_vma=False,
    )
```

```python
from functools import partial

import jax
import jax.numpy as jnp
from jax import lax
from jax.experimental import pallas as pl
from jax.experimental.pallas import tpu as pltpu
from jax.sharding import PartitionSpec as P

EPSILON = 1e-05
MESH = pl.DeviceIdType.MESH
BLOCK = 256
PIECE = 16
LOWEST = -3e38
F32 = jnp.float32
BF16 = jnp.bfloat16


def transfers(face_len):
    low, high = 0, face_len
    edge = face_len - PIECE
    end = PIECE + face_len
    return (
        (1, 0, high, face_len, 0, 0),
        (-1, 0, low, face_len, 0, face_len),
        (0, 1, 3 * face_len, face_len, 1, PIECE),
        (0, -1, 2 * face_len, face_len, 2, PIECE),
        (1, 1, high + edge, PIECE, 1, 0),
        (-1, 1, low + edge, PIECE, 1, end),
        (1, -1, high, PIECE, 2, 0),
        (-1, -1, low, PIECE, 2, end),
    )


def tap_of(dx, dy, z):
    return 9 * (dx + 1) + 3 * (dy + 1) + z


def plane_size(n_slab):
    size = 1
    while 4 * size * size <= n_slab and n_slab % (2 * size) == 0:
        size *= 2
    return size


def block_kernel(
    n_slab,
    n_tile,
    feat_hbm,
    rule_hbm,
    face_hbm,
    gain_one_hbm,
    shift_one_hbm,
    gain_two_hbm,
    shift_two_hbm,
    conv_one_hbm,
    conv_two_hbm,
    out_ref,
    feat_ref,
    rule_ref,
    face_ref,
    gain_one_ref,
    shift_one_ref,
    gain_two_ref,
    shift_two_ref,
    weight_ref,
    weight_t_ref,
    side_weight_ref,
    onehot_ref,
    hot_ref,
    place_ref,
    part_ref,
    keep_ref,
    face_hot_ref,
    square_ref,
    corner_ref,
    edge_ref,
    side_ref,
    acc_ref,
    own_ref,
    send_ref,
    wide_send_ref,
    halo_ref,
    wide_halo_ref,
    lhs_ref,
    picked_ref,
    stats_one_ref,
    stats_two_ref,
    input_sem,
    send_sem,
    recv_sem,
    stat_send_sem,
    stat_recv_sem,
    ready_sem,
):
    rows, channels = feat_ref.shape
    taps = rule_ref.shape[0]
    face_len = face_ref.shape[1]
    side = rows // face_len
    column = face_len // side
    n_dev = n_slab * n_tile
    blocks = rows // BLOCK
    half = taps // 2
    wide = 2 * face_len
    slab = lax.axis_index("slab")
    tile = lax.axis_index("tile")
    me = slab * n_tile + tile

    def fetch(i, src, dst):
        return pltpu.make_async_copy(src, dst, input_sem.at[i])

    feat_copy = fetch(0, feat_hbm, feat_ref)
    face_copy = fetch(1, face_hbm, face_ref)
    rule_copy = fetch(2, rule_hbm, rule_ref)
    affine_copies = [
        fetch(3, gain_one_hbm, gain_one_ref),
        fetch(4, shift_one_hbm, shift_one_ref),
        fetch(5, gain_two_hbm, gain_two_ref),
        fetch(6, shift_two_hbm, shift_two_ref),
    ]
    weight_copies = [
        fetch(7, conv_one_hbm, weight_ref.at[0]),
        fetch(8, conv_two_hbm, weight_ref.at[1]),
    ]
    for copy in (face_copy, feat_copy, rule_copy):
        copy.start()
    halo_ref[...] = jnp.zeros_like(halo_ref)
    wide_halo_ref[...] = jnp.zeros_like(wide_halo_ref)

    def moved(place, step, size):
        if size & (size - 1) == 0:
            return place ^ step
        place = place + step
        return jnp.where(place >= size, place - size, place)

    def each_peer(act):
        for j in reversed(range(n_tile)):
            other = moved(tile, j, n_tile) if j else tile

            def visit(i, carry):
                act({"slab": moved(slab, n_slab - 1 - i, n_slab), "tile": other})
                return carry

            last = n_slab if j else n_slab - 1
            lax.fori_loop(0, last, visit, 0, unroll=n_slab <= 16)

    plane = plane_size(n_slab)
    within = slab % plane
    first_of_plane = slab - within

    def each_near(act):
        for i in range(n_slab // plane - 1, 0, -1):
            layer = moved(slab // plane, i, n_slab // plane)
            act({"slab": layer * plane + within, "tile": tile})
        for step, crosses in ((1, within == plane - 1), (-1, within == 0)):
            inside = (slab + step >= 0) & (slab + step < n_slab)
            for dt in (-1, 0, 1):
                there = inside & crosses & (tile + dt >= 0) & (tile + dt < n_tile)
                peer = {"slab": slab + step, "tile": tile + dt}
                pl.when(there)(partial(act, peer))
        for i in range(plane - 1, -1, -1):
            for j in range(n_tile - 1, -1, -1):
                if i or j:
                    other = first_of_plane + moved(within, i, plane)
                    act({"slab": other, "tile": moved(tile, j, n_tile) if j else tile})

    near_tiles = 1 + (tile > 0).astype(jnp.int32) + (tile < n_tile - 1).astype(jnp.int32)
    crossings = ((within == 0) & (slab > 0)).astype(jnp.int32) + (
        (within == plane - 1) & (slab < n_slab - 1)
    ).astype(jnp.int32)
    n_near = n_slab // plane - 1 + plane * n_tile - 1 + crossings * near_tiles

    barrier = pltpu.get_barrier_semaphore()
    each_near(
        lambda peer: pl.semaphore_signal(barrier, inc=1, device_id=peer, device_id_type=MESH)
    )
    for copy in weight_copies + affine_copies:
        copy.start()

    def halo(which, start):
        source, target = ((send_ref, halo_ref), (wide_send_ref, wide_halo_ref))[which]
        for j, (ds, dt, first, size, buffer, place) in enumerate(transfers(face_len)):
            copy = pltpu.make_async_remote_copy(
                src_ref=source.at[pl.ds(first, size)],
                dst_ref=target.at[buffer, pl.ds(place, size)],
                send_sem=send_sem.at[which, j],
                recv_sem=recv_sem.at[which, j],
                device_id={"slab": slab + ds, "tile": tile + dt},
                device_id_type=MESH,
            )
            sends, receives = True, True
            if ds > 0:
                sends, receives = slab < n_slab - 1, slab > 0
            elif ds < 0:
                sends, receives = slab > 0, slab < n_slab - 1
            if dt > 0:
                sends, receives = sends & (tile < n_tile - 1), receives & (tile > 0)
            elif dt < 0:
                sends, receives = sends & (tile > 0), receives & (tile < n_tile - 1)
            if start:
                pl.when(sends)(copy.start)
            else:
                pl.when(receives)(copy.wait_recv)
                pl.when(sends)(copy.wait_send)

    corner_ref[...] = jnp.zeros_like(corner_ref)
    edge_ref[...] = jnp.zeros_like(edge_ref)
    face_copy.wait()
    square_ref[...] = jnp.zeros_like(square_ref)
    square_ref[0:4, 0:face_len] = face_ref[...].astype(F32)
    face_cols = square_ref[...].T
    lane_rows = lax.broadcasted_iota(jnp.int32, (face_len, rows), 1)
    for k in range(4):
        wanted = face_cols[0:face_len, k : k + 1].astype(jnp.int32)
        face_hot_ref[k * face_len : (k + 1) * face_len, :] = jnp.where(
            lane_rows == wanted, 1.0, 0.0
        ).astype(BF16)

    feat_copy.wait()
    feat = feat_ref[...]
    send_ref[...] = jnp.dot(face_hot_ref[...], feat, preferred_element_type=F32).astype(BF16)

    pl.semaphore_wait(barrier, n_near)
    halo(0, True)
    each_near(
        lambda peer: pl.semaphore_signal(ready_sem, inc=1, device_id=peer, device_id_type=MESH)
    )

    for b in range(blocks):
        lhs_ref[b * channels : (b + 1) * channels, :] = feat[b * BLOCK : (b + 1) * BLOCK].T

    rule_copy.wait()
    rule = rule_ref[...]
    below = rows + 2 * face_len
    tile_len = face_len + 2 * column
    table = below + 2 * tile_len
    place_ref[...] = jnp.where(rule < rows, rule & (BLOCK - 1), -1).astype(F32)
    part_ref[...] = rule // BLOCK
    keep_ref[...] = jnp.where(rule < table, 1, 0)
    position = lax.broadcasted_iota(jnp.int32, (BLOCK, rows), 0).astype(F32).astype(BF16)
    one, none = jnp.ones((BLOCK, rows), BF16), jnp.zeros((BLOCK, rows), BF16)

    def hot(places, low, size):
        return jnp.where(
            position[low : low + size] == places.astype(F32).astype(BF16),
            one[0:size],
            none[0:size],
        )

    def side_hot(dx, dy, z, low):
        spot = rule_ref[tap_of(dx, dy, z)]
        places = jnp.full((1, rows), -1, jnp.int32)

        def fill(places, base, size, to):
            inside = (spot >= base) & (spot < base + size)
            return jnp.where(inside, spot - base + to, places)

        if dx:
            places = fill(places, rows + (face_len if dx > 0 else 0), face_len, low)
        if dy:
            start = below + (tile_len if dy > 0 else 0)
            places = fill(places, start + column, face_len, low + (face_len if dx else 0))
            if dx:
                end = column + face_len if dx > 0 else 0
                places = fill(
                    places, start + end, column, low + (face_len - column if dy < 0 else 0)
                )
        return hot(places, low, wide if dx and dy else face_len)

    live = keep_ref[half].astype(F32)
    count = jnp.sum(live, axis=1, keepdims=True)
    live_rows = (
        lax.broadcasted_iota(jnp.int32, (rows, 1), 0).astype(F32) < count
    ).astype(F32)

    def turn_weights(i):
        weight_copies[i].wait()
        for dx in (-1, 0, 1):
            for dy in (-1, 0, 1):
                for z in range(3):
                    tap = tap_of(dx, dy, z)
                    turned = weight_ref[i, tap * channels : (tap + 1) * channels, :].T
                    weight_t_ref[i, :, tap * channels : (tap + 1) * channels] = turned
                    if i == 0 and (dx or dy):
                        if dx and dy:
                            which, part = (dx + 1) // 2, (dy + 1) // 2
                        elif dx:
                            which, part = 2, (dx + 1) // 2
                        else:
                            which, part = 3, (dy + 1) // 2
                        side_weight_ref[
                            which,
                            z * channels : (z + 1) * channels,
                            part * channels : (part + 1) * channels,
                        ] = turned

    def choose(tap, found):
        value = found[0:channels]
        for b in range(1, blocks):
            value = jnp.where(part_ref[tap] == b, found[b * channels : (b + 1) * channels], value)
        return value

    def pick_local(build):
        def pick(h, carry):
            for j in range(half):
                tap = h * (half + 1) + j
                slot = h * half + j
                if build:
                    onehot_ref[slot] = jnp.where(position == place_ref[tap].astype(BF16), one, none)
                found = jnp.dot(lhs_ref[...], onehot_ref[slot], preferred_element_type=F32)
                picked_ref[tap] = choose(tap, found).astype(BF16)
            return carry

        lax.fori_loop(0, 2, pick, 0)

    pick_local(True)
    for b in range(blocks):
        picked_ref[half, :, b * BLOCK : (b + 1) * BLOCK] = lhs_ref[
            b * channels : (b + 1) * channels, :
        ]
    turn_weights(0)
    acc_ref[...] = jnp.dot(
        weight_t_ref[0], picked_ref[...].reshape(taps * channels, rows), preferred_element_type=F32
    )
    for z in range(3):
        for i, dx in enumerate((-1, 1)):
            for j, dy in enumerate((-1, 1)):
                hot_ref[3 * z + i, j * wide : (j + 1) * wide, :] = side_hot(dx, dy, z, j * wide)
        for j, (dx, dy) in enumerate(((-1, 0), (1, 0), (0, -1), (0, 1))):
            low = j * face_len
            hot_ref[3 * z + 2, low : low + face_len, :] = side_hot(dx, dy, z, low)

    sub = lax.broadcasted_iota(jnp.int32, (PIECE, channels), 0).astype(F32)
    ahead = (sub < column).astype(F32)

    def sides(pieces):
        slabs, low_tile, high_tile = pieces
        end = PIECE + face_len
        edge = face_len - PIECE

        def mix(upper, lower):
            dtype = upper.dtype
            upper, lower = upper.astype(F32), lower.astype(F32)
            return (upper * ahead + lower * (1.0 - ahead)).astype(dtype)

        corners, straight = [], []
        for i in range(2):
            own = slabs[i * face_len : (i + 1) * face_len]
            spot = slice(end, end + PIECE) if i else slice(0, PIECE)
            straight.append(own)
            corners.append(
                jnp.concatenate(
                    [own[0:edge], mix(own[edge:], low_tile[spot]), low_tile[PIECE:end]], axis=0
                )
            )
            corners.append(
                jnp.concatenate(
                    [mix(high_tile[spot], own[0:PIECE]), own[PIECE:], high_tile[PIECE:end]], axis=0
                )
            )
        straight.append(low_tile[PIECE:end])
        straight.append(high_tile[PIECE:end])
        return corners, straight

    across = (((1,), (1,)), ((), ()))

    def tell(which, buffer, values, more):
        kept = values * live_rows
        sums = [jnp.sum(kept, axis=0, keepdims=True), jnp.sum(kept * values, axis=0, keepdims=True)]
        buffer[me] = jnp.concatenate(sums + more, axis=0)
        mine = buffer.at[me]
        each_peer(
            lambda peer: pltpu.make_async_remote_copy(
                src_ref=mine,
                dst_ref=mine,
                send_sem=stat_send_sem.at[which],
                recv_sem=stat_recv_sem.at[which],
                device_id=peer,
                device_id_type=MESH,
            ).start()
        )
        return sums[0]

    def shared(which, buffer):
        others = buffer.at[pl.ds(0, n_dev - 1)]
        pltpu.make_async_copy(others, others, stat_recv_sem.at[which]).wait()
        pltpu.make_async_copy(others, others, stat_send_sem.at[which]).wait()
        return jnp.sum(buffer[...], axis=0)

    def spread(row):
        return jnp.broadcast_to(row, (channels, channels)).T

    def repeat(square):
        return jnp.concatenate([square] * (rows // channels), axis=1)

    halo(0, False)
    corners, straight = sides([halo_ref[i] for i in range(3)])
    for i in range(4):
        j = i % 2
        corner_ref[
            i // 2, j * wide : (j + 1) * wide, j * channels : (j + 1) * channels
        ] = corners[i]
        edge_ref[
            i // 2, j * face_len : (j + 1) * face_len, j * channels : (j + 1) * channels
        ] = straight[i]
    products = [
        lax.dot_general(
            side_weight_ref[i],
            corner_ref[i] if i < 2 else edge_ref[i - 2],
            across,
            preferred_element_type=F32,
        ).astype(BF16)
        for i in range(4)
    ]
    lhs = jnp.concatenate(
        [products[i][z * channels : (z + 1) * channels] for z in range(3) for i in range(4)], axis=1
    )
    first_t = acc_ref[...] + jnp.dot(
        lhs, hot_ref[...].reshape(9 * 2 * wide, rows), preferred_element_type=F32
    )
    acc_ref[...] = first_t
    first = first_t.T
    pl.semaphore_wait(ready_sem, n_near)
    counts = jnp.broadcast_to(count, (2, channels))
    centre = tell(0, stats_one_ref, first, [counts]) / count

    coarse = first.astype(BF16)
    fine = (first - coarse.astype(F32)).astype(BF16)
    both = jnp.dot(
        face_hot_ref[...],
        jnp.concatenate([coarse, fine], axis=1),
        preferred_element_type=F32,
    )
    wide_send_ref[...] = both[:, 0:channels] + both[:, channels:]
    halo(1, True)
    centred = acc_ref[...] - repeat(spread(centre))
    own_ref[...] = centred
    for b in range(blocks):
        lhs_ref[b * channels : (b + 1) * channels, :] = centred[
            :, b * BLOCK : (b + 1) * BLOCK
        ].astype(BF16)
    pick_local(False)
    turn_weights(1)
    for copy in affine_copies:
        copy.wait()

    def masked(tap, value):
        return jnp.where(keep_ref[tap] > 0, value, LOWEST).astype(BF16)

    for tap in (half - 1, half + 1):
        picked_ref[tap] = masked(tap, picked_ref[tap].astype(F32))
    halo(1, False)
    corners, straight = sides([(wide_halo_ref[i] - centre).astype(BF16) for i in range(3)])
    for i in range(4):
        side_ref[i] = corners[i].T
    lanes = lax.broadcasted_iota(jnp.int32, (channels, wide), 1)
    for i in range(2):
        turned = jnp.concatenate(straight[2 * i : 2 * i + 2], axis=0).astype(F32).T
        side_ref[4 + 2 * i] = jnp.where(lanes < face_len, turned, 0.0).astype(BF16)
        side_ref[5 + 2 * i] = jnp.where(lanes < face_len, 0.0, turned).astype(BF16)

    def add_side(tap, found):
        picked_ref[tap] = masked(tap, picked_ref[tap].astype(F32) + found)

    for z in range(3):
        for i, dx in enumerate((-1, 1)):
            for j, dy in enumerate((-1, 1)):
                spots = hot_ref[3 * z + i, j * wide : (j + 1) * wide, :]
                found = jnp.dot(side_ref[2 * i + j], spots, preferred_element_type=F32)
                add_side(tap_of(dx, dy, z), found)
        for i in range(2):
            spots = hot_ref[3 * z + 2, i * wide : (i + 1) * wide, :]
            pair = side_ref[4 + 2 * i : 6 + 2 * i].reshape(2 * channels, wide)
            found = jnp.dot(pair, spots, preferred_element_type=F32)
            for j, step in enumerate((-1, 1)):
                dx, dy = (0, step) if i else (step, 0)
                add_side(tap_of(dx, dy, z), found[j * channels : (j + 1) * channels])
    ratio = shift_one_ref[...] / gain_one_ref[...]

    total = shared(0, stats_one_ref)
    voxels = total[2:3]
    average = total[0:1] / voxels
    spread_one = total[1:2] / voxels - average * average + EPSILON
    inverse = lax.rsqrt(spread_one)
    scale = inverse * gain_one_ref[...]
    floor_col = spread(average - centre - ratio * (spread_one * inverse))
    scale_col = spread(scale)

    centre_value = jnp.maximum(own_ref[...], repeat(floor_col)) - repeat(floor_col)
    centre_value = jnp.where(keep_ref[half] > 0, centre_value * repeat(scale_col), 0.0)
    low = repeat(floor_col.astype(BF16))
    second_t = jnp.zeros((channels, rows), F32)
    group = taps // 3
    for x in range(3):
        taken, used = [], []
        for j in range(group):
            tap = x * group + j
            weight = weight_t_ref[1, :, tap * channels : (tap + 1) * channels]
            if tap == half:
                taken.append(centre_value.astype(BF16))
                used.append(weight)
            else:
                taken.append(jnp.maximum(picked_ref[tap], low) - low)
                used.append((weight.astype(F32) * scale).astype(BF16))
        second_t = second_t + jnp.dot(
            jnp.concatenate(used, axis=1),
            jnp.concatenate(taken, axis=0),
            preferred_element_type=F32,
        )
    second = second_t.T
    tell(1, stats_two_ref, second, [])
    total = shared(1, stats_two_ref)
    average = total[0:1] / voxels
    variance = total[1:2] / voxels - average * average
    scale = lax.rsqrt(variance + EPSILON) * gain_two_ref[...]
    offset = shift_two_ref[...] - average * scale
    summed = second * scale + offset + feat_ref[...].astype(F32)
    out_ref[...] = (live_rows * jnp.maximum(summed, 0.0)).astype(BF16)


def per_device(
    n_slab,
    n_tile,
    features,
    counts,
    rulebook,
    face_rows,
    conv_one,
    gain_one,
    shift_one,
    conv_two,
    gain_two,
    shift_two,
):
    rows, channels = features.shape[2:]
    taps = rulebook.shape[2]
    faces, face_len = face_rows.shape[2:]
    blocks = rows // BLOCK
    n_dev = n_slab * n_tile
    wide = 2 * face_len
    hbm = pl.BlockSpec(memory_space=pltpu.HBM)
    stay = partial(pltpu.with_memory_space_constraint, memory_space=pltpu.HBM)
    output = pl.pallas_call(
        partial(block_kernel, n_slab, n_tile),
        out_shape=pltpu.VMEM((rows, channels), features.dtype),
        in_specs=[hbm] * 9,
        out_specs=pl.BlockSpec(memory_space=pltpu.VMEM),
        scratch_shapes=[
            pltpu.VMEM((rows, channels), BF16),
            pltpu.VMEM((taps, 1, rows), jnp.int32),
            pltpu.VMEM((faces, face_len), jnp.int32),
            pltpu.VMEM((1, channels), F32),
            pltpu.VMEM((1, channels), F32),
            pltpu.VMEM((1, channels), F32),
            pltpu.VMEM((1, channels), F32),
            pltpu.VMEM((2, taps * channels, channels), BF16),
            pltpu.VMEM((2, channels, taps * channels), BF16),
            pltpu.VMEM((4, 3 * channels, 2 * channels), BF16),
            pltpu.VMEM((taps - 1, BLOCK, rows), BF16),
            pltpu.VMEM((9, 2 * wide, rows), BF16),
            pltpu.VMEM((taps, 1, rows), F32),
            pltpu.VMEM((taps, 1, rows), jnp.int32),
            pltpu.VMEM((taps, 1, rows), jnp.int32),
            pltpu.VMEM((faces * face_len, rows), BF16),
            pltpu.VMEM((channels, channels), F32),
            pltpu.VMEM((2, 2 * wide, 2 * channels), BF16),
            pltpu.VMEM((2, wide, 2 * channels), BF16),
            pltpu.VMEM((8, channels, wide), BF16),
            pltpu.VMEM((channels, rows), F32),
            pltpu.VMEM((channels, rows), F32),
            pltpu.VMEM((faces * face_len, channels), BF16),
            pltpu.VMEM((faces * face_len, channels), F32),
            pltpu.VMEM((3, BLOCK // 2, channels), BF16),
            pltpu.VMEM((3, BLOCK // 2, channels), F32),
            pltpu.VMEM((blocks * channels, BLOCK), BF16),
            pltpu.VMEM((taps, channels, rows), BF16),
            pltpu.VMEM((n_dev, 4, channels), F32),
            pltpu.VMEM((n_dev, 2, channels), F32),
            pltpu.SemaphoreType.DMA((9,)),
            pltpu.SemaphoreType.DMA((2, 8)),
            pltpu.SemaphoreType.DMA((2, 8)),
            pltpu.SemaphoreType.DMA((2,)),
            pltpu.SemaphoreType.DMA((2,)),
            pltpu.SemaphoreType.REGULAR,
        ],
        compiler_params=pltpu.CompilerParams(
            collective_id=0, has_side_effects=True, vmem_limit_bytes=48000000
        ),
    )(
        stay(features[0, 0]),
        stay(rulebook.reshape(taps, 1, rows)),
        stay(face_rows[0, 0]),
        stay(gain_one[None]),
        stay(shift_one[None]),
        stay(gain_two[None]),
        stay(shift_two[None]),
        stay(conv_one.reshape(taps * channels, channels)),
        stay(conv_two.reshape(taps * channels, channels)),
    )
    return output[None, None]


def solution(mesh):
    placed = (
        P("slab", "tile", None, None),
        P("slab", "tile"),
        P("slab", "tile", None, None),
        P("slab", "tile", None, None),
        P(),
        P(),
        P(),
        P(),
        P(),
        P(),
    )
    return jax.shard_map(
        partial(per_device, mesh.shape["slab"], mesh.shape["tile"]),
        mesh=mesh,
        in_specs=placed,
        out_specs=P("slab", "tile", None, None),
        check_vma=False,
    )
```

```python
from functools import partial

import jax
import jax.numpy as jnp
from jax import lax
from jax.experimental import pallas as pl
from jax.experimental.pallas import tpu as pltpu
from jax.sharding import PartitionSpec as P

EPSILON = 1e-05
MESH = pl.DeviceIdType.MESH
BLOCK = 256
PIECE = 16
LOWEST = -3e38
F32 = jnp.float32
BF16 = jnp.bfloat16


def transfers(face_len):
    low, high = 0, face_len
    edge = face_len - PIECE
    end = PIECE + face_len
    return (
        (1, 0, high, face_len, 0, 0),
        (-1, 0, low, face_len, 0, face_len),
        (0, 1, 3 * face_len, face_len, 1, PIECE),
        (0, -1, 2 * face_len, face_len, 2, PIECE),
        (1, 1, high + edge, PIECE, 1, 0),
        (-1, 1, low + edge, PIECE, 1, end),
        (1, -1, high, PIECE, 2, 0),
        (-1, -1, low, PIECE, 2, end),
    )


def tap_of(dx, dy, z):
    return 9 * (dx + 1) + 3 * (dy + 1) + z


def plane_size(n_slab):
    size = 1
    while 4 * size * size <= n_slab and n_slab % (2 * size) == 0:
        size *= 2
    return size


def block_kernel(
    n_slab,
    n_tile,
    feat_hbm,
    rule_hbm,
    face_hbm,
    gain_one_hbm,
    shift_one_hbm,
    gain_two_hbm,
    shift_two_hbm,
    conv_one_hbm,
    conv_two_hbm,
    out_ref,
    feat_ref,
    rule_ref,
    face_ref,
    gain_one_ref,
    shift_one_ref,
    gain_two_ref,
    shift_two_ref,
    weight_ref,
    weight_t_ref,
    side_weight_ref,
    onehot_ref,
    hot_ref,
    place_ref,
    part_ref,
    keep_ref,
    face_hot_ref,
    square_ref,
    corner_ref,
    edge_ref,
    side_ref,
    acc_ref,
    own_ref,
    send_ref,
    wide_send_ref,
    halo_ref,
    wide_halo_ref,
    lhs_ref,
    picked_ref,
    stats_one_ref,
    stats_two_ref,
    input_sem,
    send_sem,
    recv_sem,
    stat_send_sem,
    stat_recv_sem,
    ready_sem,
):
    rows, channels = feat_ref.shape
    taps = rule_ref.shape[0]
    face_len = face_ref.shape[1]
    side = rows // face_len
    column = face_len // side
    n_dev = n_slab * n_tile
    blocks = rows // BLOCK
    half = taps // 2
    wide = 2 * face_len
    slab = lax.axis_index("slab")
    tile = lax.axis_index("tile")
    me = slab * n_tile + tile

    def fetch(i, src, dst):
        return pltpu.make_async_copy(src, dst, input_sem.at[i])

    feat_copy = fetch(0, feat_hbm, feat_ref)
    face_copy = fetch(1, face_hbm, face_ref)
    rule_copy = fetch(2, rule_hbm, rule_ref)
    affine_copies = [
        fetch(3, gain_one_hbm, gain_one_ref),
        fetch(4, shift_one_hbm, shift_one_ref),
        fetch(5, gain_two_hbm, gain_two_ref),
        fetch(6, shift_two_hbm, shift_two_ref),
    ]
    weight_copies = [
        fetch(7, conv_one_hbm, weight_ref.at[0]),
        fetch(8, conv_two_hbm, weight_ref.at[1]),
    ]
    for copy in (face_copy, feat_copy, rule_copy):
        copy.start()
    halo_ref[...] = jnp.zeros_like(halo_ref)
    wide_halo_ref[...] = jnp.zeros_like(wide_halo_ref)

    def moved(place, step, size):
        if size & (size - 1) == 0:
            return place ^ step
        place = place + step
        return jnp.where(place >= size, place - size, place)

    plane = plane_size(n_slab)

    def each_peer(act, far):
        for j in reversed(range(n_tile)):
            other = moved(tile, j, n_tile) if j else tile
            top, least = (n_slab - 1, plane) if far else (plane - 1, 0 if j else 1)

            def visit(i, carry):
                act({"slab": moved(slab, top - i, n_slab), "tile": other})
                return carry

            lax.fori_loop(0, top + 1 - least, visit, 0, unroll=n_slab <= 16)

    within = slab % plane
    first_of_plane = slab - within

    def each_near(act):
        for i in range(n_slab // plane - 1, 0, -1):
            layer = moved(slab // plane, i, n_slab // plane)
            act({"slab": layer * plane + within, "tile": tile})
        for step, crosses in ((1, within == plane - 1), (-1, within == 0)):
            inside = (slab + step >= 0) & (slab + step < n_slab)
            for dt in (-1, 0, 1):
                there = inside & crosses & (tile + dt >= 0) & (tile + dt < n_tile)
                peer = {"slab": slab + step, "tile": tile + dt}
                pl.when(there)(partial(act, peer))
        for i in range(plane - 1, -1, -1):
            for j in range(n_tile - 1, -1, -1):
                if i or j:
                    other = first_of_plane + moved(within, i, plane)
                    act({"slab": other, "tile": moved(tile, j, n_tile) if j else tile})

    near_tiles = 1 + (tile > 0).astype(jnp.int32) + (tile < n_tile - 1).astype(jnp.int32)
    crossings = ((within == 0) & (slab > 0)).astype(jnp.int32) + (
        (within == plane - 1) & (slab < n_slab - 1)
    ).astype(jnp.int32)
    n_near = n_slab // plane - 1 + plane * n_tile - 1 + crossings * near_tiles

    barrier = pltpu.get_barrier_semaphore()
    each_near(
        lambda peer: pl.semaphore_signal(barrier, inc=1, device_id=peer, device_id_type=MESH)
    )
    for copy in weight_copies + affine_copies:
        copy.start()

    def halo(which, act, chosen):
        source, target = ((send_ref, halo_ref), (wide_send_ref, wide_halo_ref))[which]
        for j, (ds, dt, first, size, buffer, place) in enumerate(transfers(face_len)):
            if j not in chosen:
                continue
            copy = pltpu.make_async_remote_copy(
                src_ref=source.at[pl.ds(first, size)],
                dst_ref=target.at[buffer, pl.ds(place, size)],
                send_sem=send_sem.at[which, j],
                recv_sem=recv_sem.at[which, j],
                device_id={"slab": slab + ds, "tile": tile + dt},
                device_id_type=MESH,
            )
            sends, receives = True, True
            if ds > 0:
                sends, receives = slab < n_slab - 1, slab > 0
            elif ds < 0:
                sends, receives = slab > 0, slab < n_slab - 1
            if dt > 0:
                sends, receives = sends & (tile < n_tile - 1), receives & (tile > 0)
            elif dt < 0:
                sends, receives = sends & (tile > 0), receives & (tile < n_tile - 1)
            if act == "start":
                pl.when(sends)(copy.start)
            elif act == "receive":
                pl.when(receives)(copy.wait_recv)
            else:
                pl.when(sends)(copy.wait_send)

    corner_ref[...] = jnp.zeros_like(corner_ref)
    edge_ref[...] = jnp.zeros_like(edge_ref)
    face_copy.wait()
    square_ref[...] = jnp.zeros_like(square_ref)
    square_ref[0:4, 0:face_len] = face_ref[...].astype(F32)
    face_cols = square_ref[...].T
    lane_rows = lax.broadcasted_iota(jnp.int32, (face_len, rows), 1)
    for k in range(4):
        wanted = face_cols[0:face_len, k : k + 1].astype(jnp.int32)
        face_hot_ref[k * face_len : (k + 1) * face_len, :] = jnp.where(
            lane_rows == wanted, 1.0, 0.0
        ).astype(BF16)

    feat_copy.wait()
    feat = feat_ref[...]
    send_ref[...] = jnp.dot(face_hot_ref[...], feat, preferred_element_type=F32).astype(BF16)

    rule_copy.wait()
    rule = rule_ref[...]
    below = rows + 2 * face_len
    tile_len = face_len + 2 * column
    table = below + 2 * tile_len
    place_ref[...] = jnp.where(rule < rows, rule & (BLOCK - 1), -1).astype(F32)
    part_ref[...] = rule // BLOCK
    keep_ref[...] = jnp.where(rule < table, 1, 0)
    position = lax.broadcasted_iota(jnp.int32, (BLOCK, rows), 0).astype(F32).astype(BF16)
    one, none = jnp.ones((BLOCK, rows), BF16), jnp.zeros((BLOCK, rows), BF16)

    def hot(places, low, size):
        return jnp.where(
            position[low : low + size] == places.astype(F32).astype(BF16),
            one[0:size],
            none[0:size],
        )

    def side_hot(dx, dy, z, low):
        spot = rule_ref[tap_of(dx, dy, z)]
        places = jnp.full((1, rows), -1, jnp.int32)

        def fill(places, base, size, to):
            inside = (spot >= base) & (spot < base + size)
            return jnp.where(inside, spot - base + to, places)

        if dx:
            places = fill(places, rows + (face_len if dx > 0 else 0), face_len, low)
        if dy:
            start = below + (tile_len if dy > 0 else 0)
            places = fill(places, start + column, face_len, low + (face_len if dx else 0))
            if dx:
                end = column + face_len if dx > 0 else 0
                places = fill(
                    places, start + end, column, low + (face_len - column if dy < 0 else 0)
                )
        return hot(places, low, wide if dx and dy else face_len)

    live = keep_ref[half].astype(F32)
    count = jnp.sum(live, axis=1, keepdims=True)
    live_rows = (
        lax.broadcasted_iota(jnp.int32, (rows, 1), 0).astype(F32) < count
    ).astype(F32)

    pl.semaphore_wait(barrier, n_near)
    halo(0, "start", range(8))
    each_near(
        lambda peer: pl.semaphore_signal(ready_sem, inc=1, device_id=peer, device_id_type=MESH)
    )

    for b in range(blocks):
        lhs_ref[b * channels : (b + 1) * channels, :] = feat[b * BLOCK : (b + 1) * BLOCK].T

    def turn_weight(i, tap):
        dx, dy, z = tap // 9 - 1, tap // 3 % 3 - 1, tap % 3
        turned = weight_ref[i, tap * channels : (tap + 1) * channels, :].T
        weight_t_ref[i, :, tap * channels : (tap + 1) * channels] = turned
        if i == 0 and (dx or dy):
            if dx and dy:
                which, part = (dx + 1) // 2, (dy + 1) // 2
            elif dx:
                which, part = 2, (dx + 1) // 2
            else:
                which, part = 3, (dy + 1) // 2
            side_weight_ref[
                which,
                z * channels : (z + 1) * channels,
                part * channels : (part + 1) * channels,
            ] = turned

    def choose(tap, found):
        value = found[0:channels]
        for b in range(1, blocks):
            value = jnp.where(part_ref[tap] == b, found[b * channels : (b + 1) * channels], value)
        return value

    def build_side(tap):
        dx, dy, z = tap // 9 - 1, tap // 3 % 3 - 1, tap % 3
        i, j = (dx + 1) // 2, (dy + 1) // 2
        if dx and dy:
            hot_ref[3 * z + i, j * wide : (j + 1) * wide, :] = side_hot(dx, dy, z, j * wide)
        elif dx or dy:
            low = (i if dx else 2 + j) * face_len
            hot_ref[3 * z + 2, low : low + face_len, :] = side_hot(dx, dy, z, low)

    def pick_local(which):
        for tap in range(taps):
            turn_weight(which, tap)
            if tap == half:
                continue
            slot = tap - (tap > half)
            if which == 0:
                onehot_ref[slot] = jnp.where(position == place_ref[tap].astype(BF16), one, none)
                build_side(tap)
            found = jnp.dot(lhs_ref[...], onehot_ref[slot], preferred_element_type=F32)
            picked_ref[tap] = choose(tap, found).astype(BF16)

    weight_copies[0].wait()
    pick_local(0)
    for b in range(blocks):
        picked_ref[half, :, b * BLOCK : (b + 1) * BLOCK] = lhs_ref[
            b * channels : (b + 1) * channels, :
        ]
    acc_ref[...] = jnp.dot(
        weight_t_ref[0], picked_ref[...].reshape(taps * channels, rows), preferred_element_type=F32
    )

    sub = lax.broadcasted_iota(jnp.int32, (PIECE, channels), 0).astype(F32)
    ahead = (sub < column).astype(F32)

    def sides(pieces):
        slabs, low_tile, high_tile = pieces
        end = PIECE + face_len
        edge = face_len - PIECE

        def mix(upper, lower):
            dtype = upper.dtype
            upper, lower = upper.astype(F32), lower.astype(F32)
            return (upper * ahead + lower * (1.0 - ahead)).astype(dtype)

        corners, straight = [], []
        for i in range(2):
            own = slabs[i * face_len : (i + 1) * face_len]
            spot = slice(end, end + PIECE) if i else slice(0, PIECE)
            straight.append(own)
            corners.append(
                jnp.concatenate(
                    [own[0:edge], mix(own[edge:], low_tile[spot]), low_tile[PIECE:end]], axis=0
                )
            )
            corners.append(
                jnp.concatenate(
                    [mix(high_tile[spot], own[0:PIECE]), own[PIECE:], high_tile[PIECE:end]], axis=0
                )
            )
        straight.append(low_tile[PIECE:end])
        straight.append(high_tile[PIECE:end])
        return corners, straight

    across = (((1,), (1,)), ((), ()))

    def tell(buffer, values, more):
        kept = values * live_rows
        sums = [jnp.sum(kept, axis=0, keepdims=True), jnp.sum(kept * values, axis=0, keepdims=True)]
        buffer[me] = jnp.concatenate(sums + more, axis=0)
        return sums[0]

    def share(which, buffer, far):
        mine = buffer.at[me]
        each_peer(
            lambda peer: pltpu.make_async_remote_copy(
                src_ref=mine,
                dst_ref=mine,
                send_sem=stat_send_sem.at[which],
                recv_sem=stat_recv_sem.at[which],
                device_id=peer,
                device_id_type=MESH,
            ).start(),
            far,
        )

    def shared(which, buffer):
        others = buffer.at[pl.ds(0, n_dev - 1)]
        pltpu.make_async_copy(others, others, stat_recv_sem.at[which]).wait()
        pltpu.make_async_copy(others, others, stat_send_sem.at[which]).wait()
        return jnp.sum(buffer[...], axis=0)

    def spread(row):
        return jnp.broadcast_to(row, (channels, channels)).T

    def repeat(square):
        return jnp.concatenate([square] * (rows // channels), axis=1)

    halo(0, "receive", range(8))
    halo(0, "sent", range(8))
    corners, straight = sides([halo_ref[i] for i in range(3)])
    for i in range(4):
        j = i % 2
        corner_ref[
            i // 2, j * wide : (j + 1) * wide, j * channels : (j + 1) * channels
        ] = corners[i]
        edge_ref[
            i // 2, j * face_len : (j + 1) * face_len, j * channels : (j + 1) * channels
        ] = straight[i]
    products = [
        lax.dot_general(
            side_weight_ref[i],
            corner_ref[i] if i < 2 else edge_ref[i - 2],
            across,
            preferred_element_type=F32,
        ).astype(BF16)
        for i in range(4)
    ]
    lhs = jnp.concatenate(
        [products[i][z * channels : (z + 1) * channels] for z in range(3) for i in range(4)], axis=1
    )
    first_t = acc_ref[...] + jnp.dot(
        lhs, hot_ref[...].reshape(9 * 2 * wide, rows), preferred_element_type=F32
    )
    acc_ref[...] = first_t
    first = first_t.T
    pl.semaphore_wait(ready_sem, n_near)
    counts = jnp.broadcast_to(count, (2, channels))
    centre = tell(stats_one_ref, first, [counts]) / count

    coarse = first.astype(BF16)
    fine = (first - coarse.astype(F32)).astype(BF16)
    both = jnp.dot(
        face_hot_ref[...],
        jnp.concatenate([coarse, fine], axis=1),
        preferred_element_type=F32,
    )
    share(0, stats_one_ref, True)
    wide_send_ref[...] = both[:, 0:channels] + both[:, channels:]
    halo(1, "start", range(8))
    share(0, stats_one_ref, False)
    centred = acc_ref[...] - repeat(spread(centre))
    own_ref[...] = centred
    for b in range(blocks):
        lhs_ref[b * channels : (b + 1) * channels, :] = centred[
            :, b * BLOCK : (b + 1) * BLOCK
        ].astype(BF16)
    weight_copies[1].wait()
    pick_local(1)
    for copy in affine_copies:
        copy.wait()

    def masked(tap, value):
        return jnp.where(keep_ref[tap] > 0, value, LOWEST).astype(BF16)

    for tap in (half - 1, half + 1):
        picked_ref[tap] = masked(tap, picked_ref[tap].astype(F32))
    lanes = lax.broadcasted_iota(jnp.int32, (channels, wide), 1)

    def add_side(tap, found):
        picked_ref[tap] = masked(tap, picked_ref[tap].astype(F32) + found)

    def pick_straight(i, own):
        turned = jnp.concatenate(own, axis=0).astype(F32).T
        side_ref[4 + 2 * i] = jnp.where(lanes < face_len, turned, 0.0).astype(BF16)
        side_ref[5 + 2 * i] = jnp.where(lanes < face_len, 0.0, turned).astype(BF16)
        for z in range(3):
            spots = hot_ref[3 * z + 2, i * wide : (i + 1) * wide, :]
            pair = side_ref[4 + 2 * i : 6 + 2 * i].reshape(2 * channels, wide)
            found = jnp.dot(pair, spots, preferred_element_type=F32)
            for j, step in enumerate((-1, 1)):
                dx, dy = (0, step) if i else (step, 0)
                add_side(tap_of(dx, dy, z), found[j * channels : (j + 1) * channels])

    def received(i):
        return (wide_halo_ref[i] - centre).astype(BF16)

    halo(1, "receive", (2, 3))
    pick_straight(
        1, [(wide_halo_ref[i, PIECE : PIECE + face_len] - centre).astype(BF16) for i in (1, 2)]
    )
    halo(1, "receive", (0, 1))
    pick_straight(0, [received(0)])
    halo(1, "receive", (4, 5, 6, 7))
    corners, _ = sides([received(i) for i in range(3)])
    for i in range(4):
        side_ref[i] = corners[i].T
    for z in range(3):
        for i, dx in enumerate((-1, 1)):
            for j, dy in enumerate((-1, 1)):
                spots = hot_ref[3 * z + i, j * wide : (j + 1) * wide, :]
                found = jnp.dot(side_ref[2 * i + j], spots, preferred_element_type=F32)
                add_side(tap_of(dx, dy, z), found)
    halo(1, "sent", range(8))
    ratio = shift_one_ref[...] / gain_one_ref[...]

    total = shared(0, stats_one_ref)
    voxels = total[2:3]
    average = total[0:1] / voxels
    spread_one = total[1:2] / voxels - average * average + EPSILON
    inverse = lax.rsqrt(spread_one)
    scale = inverse * gain_one_ref[...]
    floor_col = spread(average - centre - ratio * (spread_one * inverse))
    scale_col = spread(scale)

    centre_value = jnp.maximum(own_ref[...], repeat(floor_col)) - repeat(floor_col)
    centre_value = jnp.where(keep_ref[half] > 0, centre_value * repeat(scale_col), 0.0)
    low = repeat(floor_col.astype(BF16))
    taken, used = [], []
    for tap in range(taps):
        weight = weight_t_ref[1, :, tap * channels : (tap + 1) * channels]
        if tap == half:
            taken.append(centre_value.astype(BF16))
            used.append(weight)
        else:
            taken.append(jnp.maximum(picked_ref[tap], low) - low)
            used.append((weight.astype(F32) * scale).astype(BF16))
    second_t = jnp.dot(
        jnp.concatenate(used, axis=1), jnp.concatenate(taken, axis=0), preferred_element_type=F32
    )
    second = second_t.T
    tell(stats_two_ref, second, [])
    share(1, stats_two_ref, True)
    share(1, stats_two_ref, False)
    total = shared(1, stats_two_ref)
    average = total[0:1] / voxels
    variance = total[1:2] / voxels - average * average
    scale = lax.rsqrt(variance + EPSILON) * gain_two_ref[...]
    offset = shift_two_ref[...] - average * scale
    summed = second * scale + offset + feat_ref[...].astype(F32)
    out_ref[...] = (live_rows * jnp.maximum(summed, 0.0)).astype(BF16)


def per_device(
    n_slab,
    n_tile,
    features,
    counts,
    rulebook,
    face_rows,
    conv_one,
    gain_one,
    shift_one,
    conv_two,
    gain_two,
    shift_two,
):
    rows, channels = features.shape[2:]
    taps = rulebook.shape[2]
    faces, face_len = face_rows.shape[2:]
    blocks = rows // BLOCK
    n_dev = n_slab * n_tile
    wide = 2 * face_len
    hbm = pl.BlockSpec(memory_space=pltpu.HBM)
    stay = partial(pltpu.with_memory_space_constraint, memory_space=pltpu.HBM)
    output = pl.pallas_call(
        partial(block_kernel, n_slab, n_tile),
        out_shape=pltpu.VMEM((rows, channels), features.dtype),
        in_specs=[hbm] * 9,
        out_specs=pl.BlockSpec(memory_space=pltpu.VMEM),
        scratch_shapes=[
            pltpu.VMEM((rows, channels), BF16),
            pltpu.VMEM((taps, 1, rows), jnp.int32),
            pltpu.VMEM((faces, face_len), jnp.int32),
            pltpu.VMEM((1, channels), F32),
            pltpu.VMEM((1, channels), F32),
            pltpu.VMEM((1, channels), F32),
            pltpu.VMEM((1, channels), F32),
            pltpu.VMEM((2, taps * channels, channels), BF16),
            pltpu.VMEM((2, channels, taps * channels), BF16),
            pltpu.VMEM((4, 3 * channels, 2 * channels), BF16),
            pltpu.VMEM((taps - 1, BLOCK, rows), BF16),
            pltpu.VMEM((9, 2 * wide, rows), BF16),
            pltpu.VMEM((taps, 1, rows), F32),
            pltpu.VMEM((taps, 1, rows), jnp.int32),
            pltpu.VMEM((taps, 1, rows), jnp.int32),
            pltpu.VMEM((faces * face_len, rows), BF16),
            pltpu.VMEM((channels, channels), F32),
            pltpu.VMEM((2, 2 * wide, 2 * channels), BF16),
            pltpu.VMEM((2, wide, 2 * channels), BF16),
            pltpu.VMEM((8, channels, wide), BF16),
            pltpu.VMEM((channels, rows), F32),
            pltpu.VMEM((channels, rows), F32),
            pltpu.VMEM((faces * face_len, channels), BF16),
            pltpu.VMEM((faces * face_len, channels), F32),
            pltpu.VMEM((3, BLOCK // 2, channels), BF16),
            pltpu.VMEM((3, BLOCK // 2, channels), F32),
            pltpu.VMEM((blocks * channels, BLOCK), BF16),
            pltpu.VMEM((taps, channels, rows), BF16),
            pltpu.VMEM((n_dev, 4, channels), F32),
            pltpu.VMEM((n_dev, 2, channels), F32),
            pltpu.SemaphoreType.DMA((9,)),
            pltpu.SemaphoreType.DMA((2, 8)),
            pltpu.SemaphoreType.DMA((2, 8)),
            pltpu.SemaphoreType.DMA((2,)),
            pltpu.SemaphoreType.DMA((2,)),
            pltpu.SemaphoreType.REGULAR,
        ],
        compiler_params=pltpu.CompilerParams(
            collective_id=0, has_side_effects=True, vmem_limit_bytes=48000000
        ),
    )(
        stay(features[0, 0]),
        stay(rulebook.reshape(taps, 1, rows)),
        stay(face_rows[0, 0]),
        stay(gain_one[None]),
        stay(shift_one[None]),
        stay(gain_two[None]),
        stay(shift_two[None]),
        stay(conv_one.reshape(taps * channels, channels)),
        stay(conv_two.reshape(taps * channels, channels)),
    )
    return output[None, None]


def solution(mesh):
    placed = (
        P("slab", "tile", None, None),
        P("slab", "tile"),
        P("slab", "tile", None, None),
        P("slab", "tile", None, None),
        P(),
        P(),
        P(),
        P(),
        P(),
        P(),
    )
    return jax.shard_map(
        partial(per_device, mesh.shape["slab"], mesh.shape["tile"]),
        mesh=mesh,
        in_specs=placed,
        out_specs=P("slab", "tile", None, None),
        check_vma=False,
    )
```

```python
from functools import partial

import jax
import jax.numpy as jnp
from jax import lax
from jax.experimental import pallas as pl
from jax.experimental.pallas import tpu as pltpu
from jax.sharding import PartitionSpec as P

EPSILON = 1e-05
MESH = pl.DeviceIdType.MESH
BLOCK = 256
PIECE = 16
LOWEST = -3e38
F32 = jnp.float32
BF16 = jnp.bfloat16


def transfers(face_len):
    low, high = 0, face_len
    edge = face_len - PIECE
    end = PIECE + face_len
    return (
        (1, 0, high, face_len, 0, 0),
        (-1, 0, low, face_len, 0, face_len),
        (0, 1, 3 * face_len, face_len, 1, PIECE),
        (0, -1, 2 * face_len, face_len, 2, PIECE),
        (1, 1, high + edge, PIECE, 1, 0),
        (-1, 1, low + edge, PIECE, 1, end),
        (1, -1, high, PIECE, 2, 0),
        (-1, -1, low, PIECE, 2, end),
    )


def tap_of(dx, dy, z):
    return 9 * (dx + 1) + 3 * (dy + 1) + z


def plane_size(n_slab):
    size = 1
    while 4 * size * size <= n_slab and n_slab % (2 * size) == 0:
        size *= 2
    return size


def block_kernel(
    n_slab,
    n_tile,
    feat_hbm,
    rule_hbm,
    face_hbm,
    gain_one_hbm,
    shift_one_hbm,
    gain_two_hbm,
    shift_two_hbm,
    conv_one_hbm,
    conv_two_hbm,
    out_ref,
    feat_ref,
    rule_ref,
    face_ref,
    gain_one_ref,
    shift_one_ref,
    gain_two_ref,
    shift_two_ref,
    weight_ref,
    weight_t_ref,
    side_weight_ref,
    onehot_ref,
    hot_ref,
    place_ref,
    part_ref,
    keep_ref,
    face_hot_ref,
    square_ref,
    corner_ref,
    edge_ref,
    side_ref,
    acc_ref,
    own_ref,
    send_ref,
    wide_send_ref,
    halo_ref,
    wide_halo_ref,
    lhs_ref,
    picked_ref,
    stats_one_ref,
    stats_two_ref,
    input_sem,
    send_sem,
    recv_sem,
    stat_send_sem,
    stat_recv_sem,
    ready_sem,
):
    rows, channels = feat_ref.shape
    taps = rule_ref.shape[0]
    face_len = face_ref.shape[1]
    side = rows // face_len
    column = face_len // side
    n_dev = n_slab * n_tile
    blocks = rows // BLOCK
    half = taps // 2
    wide = 2 * face_len
    slab = lax.axis_index("slab")
    tile = lax.axis_index("tile")
    me = slab * n_tile + tile

    def fetch(i, src, dst):
        return pltpu.make_async_copy(src, dst, input_sem.at[i])

    feat_copy = fetch(0, feat_hbm, feat_ref)
    face_copy = fetch(1, face_hbm, face_ref)
    rule_copy = fetch(2, rule_hbm, rule_ref)
    affine_copies = [
        fetch(3, gain_one_hbm, gain_one_ref),
        fetch(4, shift_one_hbm, shift_one_ref),
        fetch(5, gain_two_hbm, gain_two_ref),
        fetch(6, shift_two_hbm, shift_two_ref),
    ]
    weight_copies = [
        fetch(7, conv_one_hbm, weight_ref.at[0]),
        fetch(8, conv_two_hbm, weight_ref.at[1]),
    ]
    for copy in (face_copy, feat_copy, rule_copy):
        copy.start()
    halo_ref[...] = jnp.zeros_like(halo_ref)
    wide_halo_ref[...] = jnp.zeros_like(wide_halo_ref)

    def moved(place, step, size):
        if size & (size - 1) == 0:
            return place ^ step
        place = place + step
        return jnp.where(place >= size, place - size, place)

    plane = plane_size(n_slab)

    def each_peer(act, far):
        for j in reversed(range(n_tile)):
            other = moved(tile, j, n_tile) if j else tile
            top, least = (n_slab - 1, plane) if far else (plane - 1, 0 if j else 1)

            def visit(i, carry):
                act({"slab": moved(slab, top - i, n_slab), "tile": other})
                return carry

            lax.fori_loop(0, top + 1 - least, visit, 0, unroll=n_slab <= 16)

    within = slab % plane
    first_of_plane = slab - within

    def each_near(act):
        for i in range(n_slab // plane - 1, 0, -1):
            layer = moved(slab // plane, i, n_slab // plane)
            act({"slab": layer * plane + within, "tile": tile})
        for step, crosses in ((1, within == plane - 1), (-1, within == 0)):
            inside = (slab + step >= 0) & (slab + step < n_slab)
            for dt in (-1, 0, 1):
                there = inside & crosses & (tile + dt >= 0) & (tile + dt < n_tile)
                peer = {"slab": slab + step, "tile": tile + dt}
                pl.when(there)(partial(act, peer))
        for i in range(plane - 1, -1, -1):
            for j in range(n_tile - 1, -1, -1):
                if i or j:
                    other = first_of_plane + moved(within, i, plane)
                    act({"slab": other, "tile": moved(tile, j, n_tile) if j else tile})

    near_tiles = 1 + (tile > 0).astype(jnp.int32) + (tile < n_tile - 1).astype(jnp.int32)
    crossings = ((within == 0) & (slab > 0)).astype(jnp.int32) + (
        (within == plane - 1) & (slab < n_slab - 1)
    ).astype(jnp.int32)
    n_near = n_slab // plane - 1 + plane * n_tile - 1 + crossings * near_tiles

    barrier = pltpu.get_barrier_semaphore()
    each_near(
        lambda peer: pl.semaphore_signal(barrier, inc=1, device_id=peer, device_id_type=MESH)
    )
    for copy in weight_copies + affine_copies:
        copy.start()

    def halo(which, act, chosen):
        source, target = ((send_ref, halo_ref), (wide_send_ref, wide_halo_ref))[which]
        for j, (ds, dt, first, size, buffer, place) in enumerate(transfers(face_len)):
            if j not in chosen:
                continue
            copy = pltpu.make_async_remote_copy(
                src_ref=source.at[pl.ds(first, size)],
                dst_ref=target.at[buffer, pl.ds(place, size)],
                send_sem=send_sem.at[which, j],
                recv_sem=recv_sem.at[which, j],
                device_id={"slab": slab + ds, "tile": tile + dt},
                device_id_type=MESH,
            )
            sends, receives = True, True
            if ds > 0:
                sends, receives = slab < n_slab - 1, slab > 0
            elif ds < 0:
                sends, receives = slab > 0, slab < n_slab - 1
            if dt > 0:
                sends, receives = sends & (tile < n_tile - 1), receives & (tile > 0)
            elif dt < 0:
                sends, receives = sends & (tile > 0), receives & (tile < n_tile - 1)
            if act == "start":
                pl.when(sends)(copy.start)
            elif act == "receive":
                pl.when(receives)(copy.wait_recv)
            else:
                pl.when(sends)(copy.wait_send)

    corner_ref[...] = jnp.zeros_like(corner_ref)
    edge_ref[...] = jnp.zeros_like(edge_ref)
    face_copy.wait()
    square_ref[...] = jnp.zeros_like(square_ref)
    square_ref[0:4, 0:face_len] = face_ref[...].astype(F32)
    face_cols = square_ref[...].T
    lane_rows = lax.broadcasted_iota(jnp.int32, (face_len, rows), 1)
    for k in range(4):
        wanted = face_cols[0:face_len, k : k + 1].astype(jnp.int32)
        face_hot_ref[k * face_len : (k + 1) * face_len, :] = jnp.where(
            lane_rows == wanted, 1.0, 0.0
        ).astype(BF16)

    feat_copy.wait()
    feat = feat_ref[...]
    send_ref[...] = jnp.dot(face_hot_ref[...], feat, preferred_element_type=F32).astype(BF16)

    pl.semaphore_wait(barrier, n_near)
    halo(0, "start", range(8))
    each_near(
        lambda peer: pl.semaphore_signal(ready_sem, inc=1, device_id=peer, device_id_type=MESH)
    )

    rule_copy.wait()
    rule = rule_ref[...]
    below = rows + 2 * face_len
    tile_len = face_len + 2 * column
    table = below + 2 * tile_len
    place_ref[...] = jnp.where(rule < rows, rule & (BLOCK - 1), -1).astype(F32)
    part_ref[...] = rule // BLOCK
    keep_ref[...] = jnp.where(rule < table, 1, 0)
    position = lax.broadcasted_iota(jnp.int32, (BLOCK, rows), 0).astype(F32).astype(BF16)
    one, none = jnp.ones((BLOCK, rows), BF16), jnp.zeros((BLOCK, rows), BF16)

    def hot(places, low, size):
        return jnp.where(
            position[low : low + size] == places.astype(F32).astype(BF16),
            one[0:size],
            none[0:size],
        )

    def side_hot(dx, dy, z, low):
        spot = rule_ref[tap_of(dx, dy, z)]
        places = jnp.full((1, rows), -1, jnp.int32)

        def fill(places, base, size, to):
            inside = (spot >= base) & (spot < base + size)
            return jnp.where(inside, spot - base + to, places)

        if dx:
            places = fill(places, rows + (face_len if dx > 0 else 0), face_len, low)
        if dy:
            start = below + (tile_len if dy > 0 else 0)
            places = fill(places, start + column, face_len, low + (face_len if dx else 0))
            if dx:
                end = column + face_len if dx > 0 else 0
                places = fill(
                    places, start + end, column, low + (face_len - column if dy < 0 else 0)
                )
        return hot(places, low, wide if dx and dy else face_len)

    live = keep_ref[half].astype(F32)
    count = jnp.sum(live, axis=1, keepdims=True)
    live_rows = (
        lax.broadcasted_iota(jnp.int32, (rows, 1), 0).astype(F32) < count
    ).astype(F32)

    for b in range(blocks):
        lhs_ref[b * channels : (b + 1) * channels, :] = feat[b * BLOCK : (b + 1) * BLOCK].T

    def turn_weight(i, tap):
        dx, dy, z = tap // 9 - 1, tap // 3 % 3 - 1, tap % 3
        turned = weight_ref[i, tap * channels : (tap + 1) * channels, :].T
        weight_t_ref[i, :, tap * channels : (tap + 1) * channels] = turned
        if i == 0 and (dx or dy):
            if dx and dy:
                which, part = (dx + 1) // 2, (dy + 1) // 2
            elif dx:
                which, part = 2, (dx + 1) // 2
            else:
                which, part = 3, (dy + 1) // 2
            side_weight_ref[
                which,
                z * channels : (z + 1) * channels,
                part * channels : (part + 1) * channels,
            ] = turned

    def choose(tap, found):
        value = found[0:channels]
        for b in range(1, blocks):
            value = jnp.where(part_ref[tap] == b, found[b * channels : (b + 1) * channels], value)
        return value

    def build_side(tap):
        dx, dy, z = tap // 9 - 1, tap // 3 % 3 - 1, tap % 3
        i, j = (dx + 1) // 2, (dy + 1) // 2
        if dx and dy:
            hot_ref[3 * z + i, j * wide : (j + 1) * wide, :] = side_hot(dx, dy, z, j * wide)
        elif dx or dy:
            low = (i if dx else 2 + j) * face_len
            hot_ref[3 * z + 2, low : low + face_len, :] = side_hot(dx, dy, z, low)

    def pick_local(which):
        for tap in range(taps):
            turn_weight(which, tap)
            if tap == half:
                continue
            slot = tap - (tap > half)
            if which == 0:
                onehot_ref[slot] = jnp.where(position == place_ref[tap].astype(BF16), one, none)
                build_side(tap)
            found = jnp.dot(lhs_ref[...], onehot_ref[slot], preferred_element_type=F32)
            picked_ref[tap] = choose(tap, found).astype(BF16)

    weight_copies[0].wait()
    pick_local(0)
    for b in range(blocks):
        picked_ref[half, :, b * BLOCK : (b + 1) * BLOCK] = lhs_ref[
            b * channels : (b + 1) * channels, :
        ]
    acc_ref[...] = jnp.dot(
        weight_t_ref[0], picked_ref[...].reshape(taps * channels, rows), preferred_element_type=F32
    )

    sub = lax.broadcasted_iota(jnp.int32, (PIECE, channels), 0).astype(F32)
    ahead = (sub < column).astype(F32)

    def sides(pieces):
        slabs, low_tile, high_tile = pieces
        end = PIECE + face_len
        edge = face_len - PIECE

        def mix(upper, lower):
            dtype = upper.dtype
            upper, lower = upper.astype(F32), lower.astype(F32)
            return (upper * ahead + lower * (1.0 - ahead)).astype(dtype)

        corners, straight = [], []
        for i in range(2):
            own = slabs[i * face_len : (i + 1) * face_len]
            spot = slice(end, end + PIECE) if i else slice(0, PIECE)
            straight.append(own)
            corners.append(
                jnp.concatenate(
                    [own[0:edge], mix(own[edge:], low_tile[spot]), low_tile[PIECE:end]], axis=0
                )
            )
            corners.append(
                jnp.concatenate(
                    [mix(high_tile[spot], own[0:PIECE]), own[PIECE:], high_tile[PIECE:end]], axis=0
                )
            )
        straight.append(low_tile[PIECE:end])
        straight.append(high_tile[PIECE:end])
        return corners, straight

    across = (((1,), (1,)), ((), ()))

    def tell(buffer, values, more):
        kept = values * live_rows
        sums = [jnp.sum(kept, axis=0, keepdims=True), jnp.sum(kept * values, axis=0, keepdims=True)]
        buffer[me] = jnp.concatenate(sums + more, axis=0)
        return sums[0]

    def fold(values):
        parts = [values[:, i : i + channels] for i in range(0, rows, channels)]
        while len(parts) > 1:
            parts = [sum(parts[i : i + 2]) for i in range(0, len(parts), 2)]
        return parts[0]

    def share(which, buffer, far):
        mine = buffer.at[me]
        each_peer(
            lambda peer: pltpu.make_async_remote_copy(
                src_ref=mine,
                dst_ref=mine,
                send_sem=stat_send_sem.at[which],
                recv_sem=stat_recv_sem.at[which],
                device_id=peer,
                device_id_type=MESH,
            ).start(),
            far,
        )

    def shared(which, buffer):
        others = buffer.at[pl.ds(0, n_dev - 1)]
        pltpu.make_async_copy(others, others, stat_recv_sem.at[which]).wait()
        pltpu.make_async_copy(others, others, stat_send_sem.at[which]).wait()
        return jnp.sum(buffer[...], axis=0)

    def spread(row):
        return jnp.broadcast_to(row, (channels, channels)).T

    def repeat(square):
        return jnp.concatenate([square] * (rows // channels), axis=1)

    halo(0, "receive", range(8))
    halo(0, "sent", range(8))
    corners, straight = sides([halo_ref[i] for i in range(3)])
    for i in range(4):
        j = i % 2
        corner_ref[
            i // 2, j * wide : (j + 1) * wide, j * channels : (j + 1) * channels
        ] = corners[i]
        edge_ref[
            i // 2, j * face_len : (j + 1) * face_len, j * channels : (j + 1) * channels
        ] = straight[i]
    products = [
        lax.dot_general(
            side_weight_ref[i],
            corner_ref[i] if i < 2 else edge_ref[i - 2],
            across,
            preferred_element_type=F32,
        ).astype(BF16)
        for i in range(4)
    ]
    lhs = jnp.concatenate(
        [products[i][z * channels : (z + 1) * channels] for z in range(3) for i in range(4)], axis=1
    )
    first_t = acc_ref[...] + jnp.dot(
        lhs, hot_ref[...].reshape(9 * 2 * wide, rows), preferred_element_type=F32
    )
    acc_ref[...] = first_t
    first = first_t.T
    pl.semaphore_wait(ready_sem, n_near)
    counts = jnp.broadcast_to(count, (2, channels))
    centre = tell(stats_one_ref, first, [counts]) / count

    coarse = first.astype(BF16)
    fine = (first - coarse.astype(F32)).astype(BF16)
    both = jnp.dot(
        face_hot_ref[...],
        jnp.concatenate([coarse, fine], axis=1),
        preferred_element_type=F32,
    )
    share(0, stats_one_ref, True)
    wide_send_ref[...] = both[:, 0:channels] + both[:, channels:]
    halo(1, "start", range(8))
    share(0, stats_one_ref, False)
    centred = acc_ref[...] - repeat(spread(centre))
    own_ref[...] = centred
    for b in range(blocks):
        lhs_ref[b * channels : (b + 1) * channels, :] = centred[
            :, b * BLOCK : (b + 1) * BLOCK
        ].astype(BF16)
    weight_copies[1].wait()
    pick_local(1)
    for copy in affine_copies:
        copy.wait()

    def masked(tap, value):
        return jnp.where(keep_ref[tap] > 0, value, LOWEST).astype(BF16)

    for tap in (half - 1, half + 1):
        picked_ref[tap] = masked(tap, picked_ref[tap].astype(F32))
    lanes = lax.broadcasted_iota(jnp.int32, (channels, wide), 1)

    def add_side(tap, found):
        picked_ref[tap] = masked(tap, picked_ref[tap].astype(F32) + found)

    def pick_straight(i, own):
        turned = jnp.concatenate(own, axis=0).astype(F32).T
        side_ref[4 + 2 * i] = jnp.where(lanes < face_len, turned, 0.0).astype(BF16)
        side_ref[5 + 2 * i] = jnp.where(lanes < face_len, 0.0, turned).astype(BF16)
        for z in range(3):
            spots = hot_ref[3 * z + 2, i * wide : (i + 1) * wide, :]
            pair = side_ref[4 + 2 * i : 6 + 2 * i].reshape(2 * channels, wide)
            found = jnp.dot(pair, spots, preferred_element_type=F32)
            for j, step in enumerate((-1, 1)):
                dx, dy = (0, step) if i else (step, 0)
                add_side(tap_of(dx, dy, z), found[j * channels : (j + 1) * channels])

    def received(i):
        return (wide_halo_ref[i] - centre).astype(BF16)

    halo(1, "receive", (2, 3))
    pick_straight(
        1, [(wide_halo_ref[i, PIECE : PIECE + face_len] - centre).astype(BF16) for i in (1, 2)]
    )
    halo(1, "receive", (0, 1))
    pick_straight(0, [received(0)])
    halo(1, "receive", (4, 5, 6, 7))
    corners, _ = sides([received(i) for i in range(3)])
    for i in range(4):
        side_ref[i] = corners[i].T
    for z in range(3):
        for i, dx in enumerate((-1, 1)):
            for j, dy in enumerate((-1, 1)):
                spots = hot_ref[3 * z + i, j * wide : (j + 1) * wide, :]
                found = jnp.dot(side_ref[2 * i + j], spots, preferred_element_type=F32)
                add_side(tap_of(dx, dy, z), found)
    halo(1, "sent", range(8))
    ratio = shift_one_ref[...] / gain_one_ref[...]

    total = shared(0, stats_one_ref)
    voxels = total[2:3]
    average = total[0:1] / voxels
    spread_one = total[1:2] / voxels - average * average + EPSILON
    inverse = lax.rsqrt(spread_one)
    scale = inverse * gain_one_ref[...]
    floor_col = spread(average - centre - ratio * (spread_one * inverse))
    scale_col = spread(scale)

    centre_value = jnp.maximum(own_ref[...], repeat(floor_col)) - repeat(floor_col)
    centre_value = jnp.where(keep_ref[half] > 0, centre_value * repeat(scale_col), 0.0)
    low = repeat(floor_col.astype(BF16))
    taken, used = [], []
    for tap in range(taps):
        weight = weight_t_ref[1, :, tap * channels : (tap + 1) * channels]
        if tap == half:
            taken.append(centre_value.astype(BF16))
            used.append(weight)
        else:
            taken.append(jnp.maximum(picked_ref[tap], low) - low)
            used.append((weight.astype(F32) * scale).astype(BF16))
    second_t = jnp.dot(
        jnp.concatenate(used, axis=1), jnp.concatenate(taken, axis=0), preferred_element_type=F32
    )
    kept = second_t * live
    sums = jnp.sum(
        jnp.concatenate([fold(kept), fold(kept * second_t)], axis=0).T, axis=0, keepdims=True
    )
    stats_two_ref[me] = jnp.concatenate([sums[:, 0:channels], sums[:, channels:]], axis=0)
    share(1, stats_two_ref, True)
    share(1, stats_two_ref, False)
    second = second_t.T
    total = shared(1, stats_two_ref)
    average = total[0:1] / voxels
    variance = total[1:2] / voxels - average * average
    scale = lax.rsqrt(variance + EPSILON) * gain_two_ref[...]
    offset = shift_two_ref[...] - average * scale
    summed = second * scale + offset + feat_ref[...].astype(F32)
    out_ref[...] = (live_rows * jnp.maximum(summed, 0.0)).astype(BF16)


def per_device(
    n_slab,
    n_tile,
    features,
    counts,
    rulebook,
    face_rows,
    conv_one,
    gain_one,
    shift_one,
    conv_two,
    gain_two,
    shift_two,
):
    rows, channels = features.shape[2:]
    taps = rulebook.shape[2]
    faces, face_len = face_rows.shape[2:]
    blocks = rows // BLOCK
    n_dev = n_slab * n_tile
    wide = 2 * face_len
    hbm = pl.BlockSpec(memory_space=pltpu.HBM)
    stay = partial(pltpu.with_memory_space_constraint, memory_space=pltpu.HBM)
    output = pl.pallas_call(
        partial(block_kernel, n_slab, n_tile),
        out_shape=pltpu.VMEM((rows, channels), features.dtype),
        in_specs=[hbm] * 9,
        out_specs=pl.BlockSpec(memory_space=pltpu.VMEM),
        scratch_shapes=[
            pltpu.VMEM((rows, channels), BF16),
            pltpu.VMEM((taps, 1, rows), jnp.int32),
            pltpu.VMEM((faces, face_len), jnp.int32),
            pltpu.VMEM((1, channels), F32),
            pltpu.VMEM((1, channels), F32),
            pltpu.VMEM((1, channels), F32),
            pltpu.VMEM((1, channels), F32),
            pltpu.VMEM((2, taps * channels, channels), BF16),
            pltpu.VMEM((2, channels, taps * channels), BF16),
            pltpu.VMEM((4, 3 * channels, 2 * channels), BF16),
            pltpu.VMEM((taps - 1, BLOCK, rows), BF16),
            pltpu.VMEM((9, 2 * wide, rows), BF16),
            pltpu.VMEM((taps, 1, rows), F32),
            pltpu.VMEM((taps, 1, rows), jnp.int32),
            pltpu.VMEM((taps, 1, rows), jnp.int32),
            pltpu.VMEM((faces * face_len, rows), BF16),
            pltpu.VMEM((channels, channels), F32),
            pltpu.VMEM((2, 2 * wide, 2 * channels), BF16),
            pltpu.VMEM((2, wide, 2 * channels), BF16),
            pltpu.VMEM((8, channels, wide), BF16),
            pltpu.VMEM((channels, rows), F32),
            pltpu.VMEM((channels, rows), F32),
            pltpu.VMEM((faces * face_len, channels), BF16),
            pltpu.VMEM((faces * face_len, channels), F32),
            pltpu.VMEM((3, BLOCK // 2, channels), BF16),
            pltpu.VMEM((3, BLOCK // 2, channels), F32),
            pltpu.VMEM((blocks * channels, BLOCK), BF16),
            pltpu.VMEM((taps, channels, rows), BF16),
            pltpu.VMEM((n_dev, 4, channels), F32),
            pltpu.VMEM((n_dev, 2, channels), F32),
            pltpu.SemaphoreType.DMA((9,)),
            pltpu.SemaphoreType.DMA((2, 8)),
            pltpu.SemaphoreType.DMA((2, 8)),
            pltpu.SemaphoreType.DMA((2,)),
            pltpu.SemaphoreType.DMA((2,)),
            pltpu.SemaphoreType.REGULAR,
        ],
        compiler_params=pltpu.CompilerParams(
            collective_id=0, has_side_effects=True, vmem_limit_bytes=48000000
        ),
    )(
        stay(features[0, 0]),
        stay(rulebook.reshape(taps, 1, rows)),
        stay(face_rows[0, 0]),
        stay(gain_one[None]),
        stay(shift_one[None]),
        stay(gain_two[None]),
        stay(shift_two[None]),
        stay(conv_one.reshape(taps * channels, channels)),
        stay(conv_two.reshape(taps * channels, channels)),
    )
    return output[None, None]


def solution(mesh):
    placed = (
        P("slab", "tile", None, None),
        P("slab", "tile"),
        P("slab", "tile", None, None),
        P("slab", "tile", None, None),
        P(),
        P(),
        P(),
        P(),
        P(),
        P(),
    )
    return jax.shard_map(
        partial(per_device, mesh.shape["slab"], mesh.shape["tile"]),
        mesh=mesh,
        in_specs=placed,
        out_specs=P("slab", "tile", None, None),
        check_vma=False,
    )
```
